32 devices in a mesh: acq: 8 (over z, y), grp: 4 (over x, core).
Axes of the slice: x: 2, y: 2, z: 4, core: 2. Of those that a mesh axis runs over, the one named last changes fastest.
Arguments:
- tile_slabs: float32 [256, 16, 4096], P(('acq', 'grp')), may hold values from -6 to 6
- dest_rank: int32 [256, 1], replicated, may hold values from 0 to 7; in each aligned block of 8 rows (0 to 7, 8 to 15, ...) at most 2 rows name the same one
- block_slot: int32 [256], replicated, may hold values from 0 to 15
- shifts: float32 [256, 3], replicated, may hold values from 0 to 1
- blend_weight: float32 [256], replicated, may hold values from 0.25 to 4
- parent_map: int32 [512], P(('acq', 'grp')), may hold values from 0 to 63
Outputs:
- pyramid: float32 [64, 8, 8, 1024], P(('acq', 'grp'))
The draws below stay inside these ranges and needn't reach their ends.
Inputs may be any that keep to these rules, and one draw needn't show every extreme that they name: `dest_rank`: among the rows of one device, no acq index is named more than 2 times, a bound that some block reaches.
All inputs are finite; a program needn't handle non-finite values.
Results may differ from the reference program's by a relative error of at most 0.0003.
Values sent between devices are 32-bit elements; how exact they have to be, the bound alone decides.
A program may use at most 256 MiB of HBM per device.

```python
import math
import jax
import jax.numpy as jnp
import numpy as np
from jax import lax

BZ = 16
BY = 32
BX = 128
SB_DEV = 8
BLOCKS_DEV = 16
PAR_DEV = 2
CAP = 2
SUBS = 256
BLOCKS = 512
PARENTS = 64
N_ACQ = 8
N_GRP = 4


def with_ends(values, key, least, largest):
    dims = values.shape
    spot = [jax.random.randint(jax.random.fold_in(key, axis), (), 0, dims[axis]) for axis in range(len(dims))]
    values = values.at[tuple(spot)].set(least)
    longest = dims.index(max(dims))
    spot[longest] = (spot[longest] + 1) % dims[longest]
    return values.at[tuple(spot)].set(largest)


def block_scale(own_key, dims, pieces, least, top_value):
    loudness = 1.0
    for axis_at, shards_of in pieces:
        heights = jax.random.uniform(jax.random.fold_in(jax.random.fold_in(own_key, 6), axis_at), (shards_of,), jnp.float32, least / len(pieces), top_value / len(pieces))
        loudness = loudness * jnp.repeat(jnp.exp(heights), dims[axis_at] // shards_of).reshape((-1,) + (1,) * (len(dims) - 1 - axis_at))
    return loudness


def assign_block(stream_key, own, number, rows, number_of, top, most, slope):
    sequence = jax.random.permutation(stream_key, number_of)
    crowded, usual = load_shares(number_of, rows * top, most, slope, True), load_shares(number_of, rows * top, most, slope, False)
    places = jnp.arange(number_of)

    def named(sizes, offset_by):
        used = int((sizes > 0).sum())
        fixed = max(1, used // 4)
        moved = fixed + (places - fixed + offset_by * (used - fixed)) % max(1, number_of - fixed)
        return jnp.zeros((number_of,), jnp.int32).at[sequence[jnp.where(places < fixed, places, moved)]].set(jnp.asarray(sizes, jnp.int32))

    sizes = jnp.where(number % 4 == 0, named(crowded, number // 4), named(usual, number - number // 4 - 1))
    mixed = jax.random.permutation(jax.random.fold_in(own, 3), number_of)
    donor, receiver = mixed[0:number_of // 2 * 2:2], mixed[1:number_of // 2 * 2:2]
    margin = jnp.minimum(sizes[donor] - 1, most - sizes[receiver]) // 2
    margin = jnp.where((donor == sequence[0]) | (receiver == sequence[0]) | (sizes[receiver] == 0), 0, jnp.maximum(margin, 0))
    moved = jax.random.randint(jax.random.fold_in(own, 4), (number_of // 2,), 0, 1 << 20) % (margin + 1)
    sizes = sizes.at[donor].add(-moved).at[receiver].add(moved)
    members = jnp.searchsorted(jnp.cumsum(sizes), jnp.arange(rows * top), side="right").astype(jnp.int32)
    listing = members.reshape(top, rows).T
    listing = listing[jax.random.permutation(jax.random.fold_in(own, 1), rows)]
    offset_by = jax.random.randint(jax.random.fold_in(own, 2), (rows, 1), 0, top)
    return jnp.take_along_axis(listing, (jnp.arange(top)[None, :] + offset_by) % top, axis=1)


def load_shares(count, total, reach, skew, full):
    portions = [(1 << 20) // math.isqrt(standing ** skew) + 1 for standing in range(1, count + 1)]
    largest = reach if full else min(reach, max(-(-total // count), total * portions[0] // sum(portions)))
    least = 1 if total - largest >= count - 1 else 0
    holding, rest = [largest] + [least] * (count - 1), total - largest - least * (count - 1)
    while rest > 0:
        candidates = [i for i in range(1, count) if holding[i] < largest] or [i for i in range(1, count) if holding[i] < reach]
        whole, budget = sum([portions[i] for i in candidates]), rest
        for i in candidates:
            more = min(reach - holding[i], max(1, budget * portions[i] // whole), rest)
            holding[i] = holding[i] + more
            rest = rest - more
    return np.array(holding)


def centred(key, extent, deviation, reach, cuts=(), kind=jnp.bfloat16):
    drawn = jax.random.normal(key, extent, jnp.float32) * deviation
    if len(cuts) > 0:
        drawn = block_scale(key, extent, cuts, -0.22, 0.18) * drawn
    return jnp.clip(drawn, min=-reach, max=reach).astype(kind)


def setup_inputs(seed: int = 0) -> dict:
    key_list = jax.random.split(jax.random.key(seed), 7)
    tile_slabs = centred(key_list[0], (SUBS, BZ, BY * BX), 1.0, 6.0, ((0, 32),), jnp.float32)
    dest_rank_keys = jax.random.split(jax.random.fold_in(key_list[1], 1), SUBS // SB_DEV)
    dest_rank_turns = jax.random.permutation(jax.random.fold_in(key_list[1], 3), SUBS // SB_DEV)
    dest_rank = jax.vmap(lambda own, number: assign_block(jax.random.fold_in(key_list[1], 2), own, number, SB_DEV, N_ACQ, 1, CAP, 2))(dest_rank_keys, dest_rank_turns).reshape((SUBS, 1))
    block_slot = with_ends(jax.random.randint(key_list[2], (SUBS,), 0, BLOCKS_DEV), jax.random.fold_in(key_list[2], 1), 0, BLOCKS_DEV - 1).astype(jnp.int32)
    shifts = jnp.clip(jax.random.uniform(key_list[3], (SUBS, 3), jnp.float32, 0.0, 1.0), 0.0, 1.0)
    blend_weight = jnp.clip(jnp.exp(jax.random.uniform(key_list[4], (SUBS,), jnp.float32, math.log(0.25), math.log(4.0))), 0.25, 4.0)
    parent_map = with_ends(jax.random.randint(key_list[5], (BLOCKS,), 0, N_GRP * PAR_DEV * 8), jax.random.fold_in(key_list[5], 1), 0, (N_GRP * PAR_DEV * 8) - 1).astype(jnp.int32)
    return {"tile_slabs": tile_slabs, "dest_rank": dest_rank, "block_slot": block_slot, "shifts": shifts, "blend_weight": blend_weight, "parent_map": parent_map}


def resample(blocks, offsets):
    frac_z = offsets[:, 0].reshape(-1, 1, 1, 1)
    frac_y = offsets[:, 1].reshape(-1, 1, 1, 1)
    frac_x = offsets[:, 2].reshape(-1, 1, 1, 1)
    ahead = jnp.concatenate([blocks[:, :, :, 1:], blocks[:, :, :, -1:]], axis=3)
    blocks = (1.0 - frac_x) * blocks + frac_x * ahead
    ahead = jnp.concatenate([blocks[:, :, 1:, :], blocks[:, :, -1:, :]], axis=2)
    blocks = (1.0 - frac_y) * blocks + frac_y * ahead
    ahead = jnp.concatenate([blocks[:, 1:, :, :], blocks[:, -1:, :, :]], axis=1)
    blocks = (1.0 - frac_z) * blocks + frac_z * ahead
    return blocks


def coarsen(blocks):
    count = blocks.shape[0]
    paired = blocks[..., 0::2] + blocks[..., 1::2]
    shaped = paired.reshape(count, BZ // 2, 2, BY // 2, 2, BX // 2)
    summed = jnp.sum(shaped, axis=(2, 4))
    return (0.125 * summed).reshape(count, -1)


def reference(tile_slabs, dest_rank, block_slot, shifts, blend_weight, parent_map):
    volume = jnp.moveaxis(tile_slabs.reshape(N_ACQ, N_GRP, SB_DEV, BZ, BY, BX), 1, 0)
    targets = jnp.moveaxis(dest_rank[:, 0].reshape(N_ACQ, N_GRP, SB_DEV), 1, 0)
    slots = jnp.moveaxis(block_slot.reshape(N_ACQ, N_GRP, SB_DEV), 1, 0)
    offsets = jnp.moveaxis(shifts.reshape(N_ACQ, N_GRP, SB_DEV, 3), 1, 0)
    weights = jnp.moveaxis(blend_weight.reshape(N_ACQ, N_GRP, SB_DEV), 1, 0)

    def one_group(args):
        cells, target, slot, offset, weight = args
        resampled = resample(cells.reshape(N_ACQ * SB_DEV, BZ, BY, BX), offset.reshape(-1, 3))
        place = (target * BLOCKS_DEV + slot).reshape(-1).astype(jnp.int32)
        rows = jnp.arange(N_ACQ * BLOCKS_DEV, dtype=jnp.int32)
        mixing = (rows[:, None] == place[None, :]).astype(jnp.float32) * weight.reshape(1, -1)
        numer = jnp.dot(mixing, resampled.reshape(N_ACQ * SB_DEV, -1), precision=lax.Precision.HIGHEST)
        denom = jnp.sum(mixing, axis=1)
        joined = numer / jnp.maximum(denom, 1.0)[:, None]
        coarse = coarsen(joined.reshape(-1, BZ, BY, BX))
        return coarse.reshape(N_ACQ, BLOCKS_DEV, -1)

    coarse_all = lax.map(one_group, (volume, targets, slots, offsets, weights))
    coarse_all = jnp.moveaxis(coarse_all, 0, 1).reshape(N_ACQ, N_GRP * BLOCKS_DEV, -1)
    parents = parent_map.reshape(N_ACQ, N_GRP * BLOCKS_DEV)

    def one_column(coarse, parent):
        rows = jnp.arange(N_GRP * PAR_DEV * 8, dtype=jnp.int32)
        placing = (rows[:, None] == parent[None, :]).astype(jnp.float32)
        return jnp.dot(placing, coarse, precision=lax.Precision.HIGHEST)

    pyramid = jax.vmap(one_column)(coarse_all, parents)
    return pyramid.reshape(PARENTS, 8, BZ // 2, (BY // 2) * (BX // 2))
```

```python
import functools
import jax
import jax.numpy as jnp
from jax import lax
from jax.experimental import pallas as pl
from jax.experimental.pallas import tpu as pltpu
from jax.sharding import PartitionSpec as P

BZ = 16
BY = 32
BX = 128
PAR_DEV = 2
HZ, HY, HX = BZ // 2, BY // 2, BX // 2
PAIRS = HY // 2
LANES = HY * HX
VMEM_LIMIT = 62
MESH = pl.DeviceIdType.MESH


def flip(index, mask, count):
    if count & (count - 1):
        return (2 * count + mask - index) % count
    out, bit = index, 1
    while bit < count:
        if mask & bit:
            out = out + bit * (1 - 2 * ((index // bit) % 2))
        bit *= 2
    return out


def partners(count):
    return list(range(1, count)) if count & (count - 1) == 0 else list(range(count))


def halving_matrix():
    row = lax.broadcasted_iota(jnp.int32, (2 * BX, 2 * BX), 0)
    col = lax.broadcasted_iota(jnp.int32, (2 * BX, 2 * BX), 1)
    x, y = row % BX, row // BX
    cx, cy, part = col % HX, (col // HX) % 2, col // BX
    same = y == cy
    both = jnp.where(same & (x // 2 == cx), 1.0, 0.0)
    ahead = jnp.where(same & (x == jnp.minimum(2 * cx + 2, BX - 1)), 1.0, 0.0)
    here = jnp.where(same & (x == 2 * cx), 1.0, 0.0)
    return jnp.where(part == 0, both, ahead - here).astype(jnp.bfloat16)


def split(values):
    high = values.astype(jnp.bfloat16)
    return high, (values - high.astype(jnp.float32)).astype(jnp.bfloat16)


def kernel(
    n_acq, n_grp, cap, tile_hbm, dest_hbm, slot_hbm, weight_hbm, shift_hbm, parent_hbm, out,
    dest, slot, weight, shift, parent, dest_row, slot_row, weight_row,
    tile, thin, high, low, half, factor, send, gath, named,
    meta_sem, load_sem, send_a, recv_a, send_x, recv_x, send_c, recv_c, send_p, recv_p,
):
    count = tile.shape[0]
    a, g = lax.axis_index("acq"), lax.axis_index("grp")
    hi, lo = g // 2, g % 2
    mate = hi * 2 + (1 - lo)
    n_hi = n_grp // 2
    rows = PAIRS * HZ

    barrier = pltpu.get_barrier_semaphore()
    for d in range(1, n_acq):
        pl.semaphore_signal(barrier, inc=1, device_id=((a + d) % n_acq, g), device_id_type=MESH)
    for d in range(1, n_grp):
        pl.semaphore_signal(barrier, inc=1, device_id=(a, (g + d) % n_grp), device_id_type=MESH)

    metas = [
        pltpu.make_async_copy(start, end, meta_sem.at[i])
        for i, (start, end) in enumerate((
            (dest_hbm, dest), (slot_hbm, slot), (weight_hbm, weight), (shift_hbm, shift),
            (parent_hbm, parent), (dest_hbm, dest_row), (slot_hbm, slot_row), (weight_hbm, weight_row),
        ))
    ]
    for meta in metas:
        meta.start()
    loads = [pltpu.make_async_copy(tile_hbm.at[s], tile.at[s], load_sem.at[s]) for s in range(count)]
    for load in loads:
        load.start()

    matrix = halving_matrix()
    last = lax.broadcasted_iota(jnp.int32, (HZ, BX), 0) == HZ - 1
    for meta in metas:
        meta.wait()

    blocks = parent.shape[1]
    base = (a * n_grp + g) * count
    target = [dest[0, base + s] for s in range(count)]
    key = [target[s] * blocks + slot[0, base + s] for s in range(count)]
    subs = lax.broadcasted_iota(jnp.int32, dest_row.shape, 1)
    keys = jnp.where(
        (subs // count) % n_grp == g, dest_row[...] * blocks + slot_row[...], -1
    )
    for s in range(count):
        denom = jnp.sum(jnp.where(keys == key[s], weight_row[...], 0.0), axis=1, keepdims=True)
        factor[s] = jnp.broadcast_to(
            (0.125 * weight[0, base + s]) / jnp.maximum(denom, 1.0), (HZ, BX)
        )
    factor[count] = jnp.zeros((HZ, BX), jnp.float32)
    spot = []
    for s in range(count):
        at = target[s] * cap
        for before in range(s):
            at = at + jnp.where(target[before] == target[s], 1, 0)
        spot.append(at)

    def soften(s, carry):
        pltpu.make_async_copy(tile_hbm.at[s], tile.at[s], load_sem.at[s]).wait()
        fz, fy = shift[0, base + s], shift[1, base + s]

        def row(y):
            return tile[s, :, pl.ds(y * BX, BX)]

        here = row(0)
        for j in range(HY):
            odd = row(2 * j + 1)
            ahead = row(2 * j + 2) if j < HY - 1 else odd
            thin[s, j] = here + odd + fy * (ahead - here)
            here = ahead
        for j in range(HY):
            even = thin[s, j, pl.ds(0, HZ, stride=2), :]
            odd = thin[s, j, pl.ds(1, HZ, stride=2), :]
            ahead = jnp.where(last, odd, pltpu.roll(even, HZ - 1, 0))
            top, rest = split(even + odd + fz * (ahead - even))
            place = (pl.ds((j // 2) * HZ, HZ), pl.ds((j % 2) * BX, BX))
            high[s, place[0], place[1]] = top.astype(jnp.float32)
            low[s, place[0], place[1]] = rest.astype(jnp.float32)
        return carry

    lax.fori_loop(0, count, soften, 0)

    def halve(s, carry):
        half[s] = jnp.dot(
            high[s].astype(jnp.bfloat16), matrix, preferred_element_type=jnp.float32
        ) + jnp.dot(low[s].astype(jnp.bfloat16), matrix, preferred_element_type=jnp.float32)
        return carry

    lax.fori_loop(0, count, halve, 0, unroll=True)
    half[count] = jnp.zeros((rows, 2 * BX), jnp.float32)

    for place in range(n_acq * cap):
        s = count
        for i in range(count):
            s = jnp.where(spot[i] == place, i, s)
        fx = shift[2, base + jnp.minimum(s, count - 1)]
        value = half[s, :, pl.ds(0, BX)] + fx * half[s, :, pl.ds(BX, BX)]
        scale = factor[s]
        for p in range(PAIRS):
            send[place // cap, pl.ds((place % cap) * HZ, HZ), pl.ds(p * BX, BX)] = scale * value[
                p * HZ : (p + 1) * HZ
            ]

    pl.semaphore_wait(barrier, n_acq - 1 + n_grp - 1)

    def to_acq(peer):
        return pltpu.make_async_remote_copy(
            src_ref=send.at[peer], dst_ref=gath.at[g, a],
            send_sem=send_a.at[peer], recv_sem=recv_a.at[a],
            device_id=(peer, g), device_id_type=MESH,
        )

    def from_acq(peer):
        return pltpu.make_async_remote_copy(
            src_ref=send.at[peer], dst_ref=gath.at[g, peer],
            send_sem=send_a.at[peer], recv_sem=recv_a.at[peer],
            device_id=(peer, g), device_id_type=MESH,
        )

    def across(owner, part, peer, sends, recvs, at):
        first, size = parts[part][1:]
        rows_ref = gath.at[owner, pl.ds(first, size)]
        return pltpu.make_async_remote_copy(
            src_ref=rows_ref, dst_ref=rows_ref,
            send_sem=sends.at[at, part], recv_sem=recvs.at[owner, part],
            device_id=(a, peer), device_id_type=MESH,
        )

    gath[g, a] = send[a]
    order = [flip(a, d, n_acq) for d in partners(n_acq)]
    for peer in order:
        to_acq(peer).start()

    steps = [a] + order
    parts = []
    for i, k in enumerate(steps):
        if i < 2 or n_acq & (n_acq - 1):
            parts.append(([i], k, 1))
        elif i % 2 == 1:
            parts.append(([i - 1, i], (k // 2) * 2, 2))

    others = [((hi + d) % n_hi) * 2 + lo for d in range(1, n_hi)]
    origins = [((hi + n_hi - d) % n_hi) * 2 + lo for d in range(1, n_hi)]
    mates = [mate] + [((hi + n_hi - d) % n_hi) * 2 + 1 - lo for d in range(1, n_hi)]

    def forward(k):
        for d, peer in enumerate(others):
            across(g, k, peer, send_x, recv_x, d).start()
        across(g, k, mate, send_c, recv_c, 0).start()

    def relay(k):
        for d, owner in enumerate(origins):
            across(owner, k, mate, send_x, recv_x, d).wait_recv()
            across(owner, k, mate, send_c, recv_c, d + 1).start()

    depth = n_acq * cap * HZ
    tall = PAR_DEV * 8 * HZ
    lane = lax.broadcasted_iota(jnp.int32, (HZ, depth), 1)

    def name(k, found):
        first = (k * n_grp + g) * count
        seen = 0
        slots = [0] * cap
        for s in range(count):
            hit = jnp.where(dest[0, first + s] == a, 1, 0)
            for c in range(cap):
                slots[c] = jnp.where(
                    (hit == 1) & (seen == c), slot[0, first + s], slots[c]
                )
            seen = seen + hit
        for c in range(cap):
            found = jnp.where(lane // HZ == k * cap + c, parent[0, slots[c]], found)
        return found

    forward(0)
    named[g] = lax.fori_loop(0, n_acq, name, jnp.zeros((HZ, depth), jnp.int32))

    def telling(d, owner, peer):
        return pltpu.make_async_remote_copy(
            src_ref=named.at[owner], dst_ref=named.at[owner],
            send_sem=send_p.at[d], recv_sem=recv_p.at[owner],
            device_id=(a, peer), device_id_type=MESH,
        )

    for d in range(1, n_grp):
        telling(d, g, (g + d) % n_grp).start()

    upright = lax.broadcasted_iota(jnp.int32, (tall, depth), 0) + g * tall
    across_lane = lax.broadcasted_iota(jnp.int32, (tall, depth), 1) % HZ

    def place_rows(owner):
        placing = jnp.where(
            named[owner, pl.ds(0, 1), :] * HZ + across_lane == upright, 1.0, 0.0
        ).astype(jnp.bfloat16)
        top, rest = split(gath[owner].reshape(depth, LANES))
        return jnp.dot(placing, top, preferred_element_type=jnp.float32) + jnp.dot(
            placing, rest, preferred_element_type=jnp.float32
        )

    for part in range(1, len(parts)):
        for i in parts[part][0]:
            from_acq(steps[i]).wait_recv()
        forward(part)
        relay(part - 1)
    out[...] = place_rows(g)
    for d in range(1, n_grp):
        owner = (g + n_grp - d) % n_grp
        telling(d, owner, owner).wait_recv()
    for k in range(len(parts)):
        across(mate, k, mate, send_c, recv_c, 0).wait_recv()
    out[...] += place_rows(mate)
    relay(len(parts) - 1)
    for owner in origins:
        out[...] += place_rows(owner)
    for owner in mates[1:]:
        for k in range(len(parts)):
            across(owner, k, mate, send_c, recv_c, 0).wait_recv()
        out[...] += place_rows(owner)

    for peer in order:
        to_acq(peer).wait_send()
    for d in range(1, n_grp):
        telling(d, g, (g + d) % n_grp).wait_send()
    for k in range(len(parts)):
        for d, peer in enumerate(others):
            across(g, k, peer, send_x, recv_x, d).wait_send()
        across(g, k, mate, send_c, recv_c, 0).wait_send()
        for d, owner in enumerate(origins):
            across(owner, k, mate, send_c, recv_c, d + 1).wait_send()


def body(tile_slabs, dest_rank, block_slot, shifts, blend_weight, parent_map):
    n_acq, n_grp = lax.axis_size("acq"), lax.axis_size("grp")
    count = tile_slabs.shape[0]
    subs = dest_rank.shape[0]
    blocks = parent_map.shape[0]
    cap = max(2, 2 * count // n_acq)
    depth = n_acq * cap * HZ
    hbm = pl.BlockSpec(memory_space=pltpu.HBM)
    rows = PAIRS * HZ
    dma = pltpu.SemaphoreType.DMA
    n_hi = n_grp // 2
    summed = pl.pallas_call(
        functools.partial(kernel, n_acq, n_grp, cap),
        out_shape=pltpu.VMEM((PAR_DEV * 8 * HZ, LANES), jnp.float32),
        in_specs=[hbm] * 6,
        out_specs=pl.BlockSpec(memory_space=pltpu.VMEM),
        scratch_shapes=[
            pltpu.SMEM((1, subs), jnp.int32),
            pltpu.SMEM((1, subs), jnp.int32),
            pltpu.SMEM((1, subs), jnp.float32),
            pltpu.SMEM((3, subs), jnp.float32),
            pltpu.SMEM((1, blocks), jnp.int32),
            pltpu.VMEM((1, subs), jnp.int32),
            pltpu.VMEM((1, subs), jnp.int32),
            pltpu.VMEM((1, subs), jnp.float32),
            pltpu.VMEM((count, BZ, BY * BX), jnp.float32),
            pltpu.VMEM((count, HY, BZ, BX), jnp.float32),
            pltpu.VMEM((count, rows, 2 * BX), jnp.float32),
            pltpu.VMEM((count, rows, 2 * BX), jnp.float32),
            pltpu.VMEM((count + 1, rows, 2 * BX), jnp.float32),
            pltpu.VMEM((count + 1, HZ, BX), jnp.float32),
            pltpu.VMEM((n_acq, cap * HZ, LANES), jnp.float32),
            pltpu.VMEM((n_grp, n_acq, cap * HZ, LANES), jnp.float32),
            pltpu.VMEM((n_grp, HZ, depth), jnp.int32),
            dma((8,)), dma((count,)),
            dma((n_acq,)), dma((n_acq,)),
            dma((max(1, n_hi - 1), n_acq)), dma((n_grp, n_acq)),
            dma((n_hi, n_acq)), dma((n_grp, n_acq)),
            dma((n_grp,)), dma((n_grp,)),
        ],
        compiler_params=pltpu.CompilerParams(
            collective_id=0, has_side_effects=True, vmem_limit_bytes=VMEM_LIMIT * 2**20
        ),
    )(
        tile_slabs, dest_rank.reshape(1, subs), block_slot.reshape(1, subs),
        blend_weight.reshape(1, subs), shifts.T, parent_map.reshape(1, blocks),
    )
    return summed.reshape(PAR_DEV, 8, HZ, LANES)


def solution(mesh):
    placed = (P(("acq", "grp"), None, None), P(), P(), P(), P(), P(("acq", "grp")))
    return jax.shard_map(
        body,
        mesh=mesh,
        in_specs=placed,
        out_specs=P(("acq", "grp"), None, None, None),
        check_vma=False,
    )
```

```python
import functools
import jax
import jax.numpy as jnp
from jax import lax
from jax.experimental import pallas as pl
from jax.experimental.pallas import tpu as pltpu
from jax.sharding import PartitionSpec as P

BZ = 16
BY = 32
BX = 128
PAR_DEV = 2
HZ, HY, HX = BZ // 2, BY // 2, BX // 2
PAIRS = HY // 2
LANES = HY * HX
VMEM_LIMIT = 62
MESH = pl.DeviceIdType.MESH


def flip(index, mask):
    out, bit = index, 1
    while bit < 64:
        out = out + bit * ((mask // bit) % 2) * (1 - 2 * ((index // bit) % 2))
        bit *= 2
    return out


def orders(count):
    unit = count // 4
    if unit < 1:
        plain = list(range(1, count))
        return [plain] * 2, [[0] + plain] * 4
    half = unit - unit // 2
    side, near, far, farther = [list(range(q * unit, (q + 1) * unit)) for q in range(4)]
    side = side[1:]
    sends = [side + near + farther + far, side + near + far + farther]
    arrivals = [
        [0] + far[:half] + side + near[:half] + farther + far[half:] + near[half:],
        [0] + side + near + far + farther,
        [0] + far[:half] + side + far[half:]
        + farther[:half] + near[:half] + farther[half:] + near[half:],
        [0] + side + near + farther[:half] + far + farther[half:],
    ]
    return sends, arrivals


def layout(index, lo, count):
    sends, arrivals = orders(count)
    unit = max(1, count // 4)
    row = index // unit
    inner = (row + row // 2) % 2 if count >= 4 else 0

    def pick(*cases):
        if len(cases) == 2:
            return cases[0] + inner * (cases[1] - cases[0])
        below, above = pick(*cases[:2]), pick(*cases[2:])
        return below + lo * (above - below)

    def landing(d, within, low):
        if (d // unit) % 4 in (1, 2):
            within = 1 - within
        return arrivals[2 * low + within].index(d)

    targets = [
        (
            pick(*pair),
            pick(*[landing(pair[within], within, low) for low in range(2) for within in range(2)]),
        )
        for pair in zip(*sends)
    ]
    return targets, [pick(*cases) for cases in zip(*arrivals)]


def halving_matrix():
    row = lax.broadcasted_iota(jnp.int32, (2 * BX, 2 * BX), 0)
    col = lax.broadcasted_iota(jnp.int32, (2 * BX, 2 * BX), 1)
    x, y = row % BX, row // BX
    cx, cy, part = col % HX, (col // HX) % 2, col // BX
    same = y == cy
    both = jnp.where(same & (x // 2 == cx), 1.0, 0.0)
    ahead = jnp.where(same & (x == jnp.minimum(2 * cx + 2, BX - 1)), 1.0, 0.0)
    here = jnp.where(same & (x == 2 * cx), 1.0, 0.0)
    return jnp.where(part == 0, both, ahead - here).astype(jnp.bfloat16)


def split(values):
    high = values.astype(jnp.bfloat16)
    return high, (values - high.astype(jnp.float32)).astype(jnp.bfloat16)


def kernel(
    n_acq, n_grp, cap, tile_hbm, dest_hbm, slot_hbm, weight_hbm, shift_hbm, parent_hbm, out,
    dest, slot, weight, shift, parent, dest_row, slot_row, weight_row,
    tile, thin, high, low, half, factor, send, gath, named,
    meta_sem, load_sem, send_a, recv_a, send_x, recv_x, send_c, recv_c, send_p, recv_p,
):
    count = tile.shape[0]
    a, g = lax.axis_index("acq"), lax.axis_index("grp")
    hi, lo = g // 2, g % 2
    mate = hi * 2 + (1 - lo)
    n_hi = n_grp // 2
    rows = PAIRS * HZ

    barrier = pltpu.get_barrier_semaphore()
    for d in range(1, n_acq):
        pl.semaphore_signal(barrier, inc=1, device_id=((a + d) % n_acq, g), device_id_type=MESH)
    for d in range(1, n_grp):
        pl.semaphore_signal(barrier, inc=1, device_id=(a, (g + d) % n_grp), device_id_type=MESH)

    metas = [
        pltpu.make_async_copy(start, end, meta_sem.at[i])
        for i, (start, end) in enumerate((
            (dest_hbm, dest), (slot_hbm, slot), (weight_hbm, weight), (shift_hbm, shift),
            (parent_hbm, parent), (dest_hbm, dest_row), (slot_hbm, slot_row), (weight_hbm, weight_row),
        ))
    ]
    for meta in metas:
        meta.start()
    loads = [pltpu.make_async_copy(tile_hbm.at[s], tile.at[s], load_sem.at[s]) for s in range(count)]
    for load in loads:
        load.start()

    matrix = halving_matrix()
    last = lax.broadcasted_iota(jnp.int32, (HZ, BX), 0) == HZ - 1
    for meta in metas:
        meta.wait()

    blocks = parent.shape[1]
    base = (a * n_grp + g) * count
    target = [dest[0, base + s] for s in range(count)]
    key = [target[s] * blocks + slot[0, base + s] for s in range(count)]
    subs = lax.broadcasted_iota(jnp.int32, dest_row.shape, 1)
    keys = jnp.where(
        (subs // count) % n_grp == g, dest_row[...] * blocks + slot_row[...], -1
    )
    for s in range(count):
        denom = jnp.sum(jnp.where(keys == key[s], weight_row[...], 0.0), axis=1, keepdims=True)
        factor[s] = jnp.broadcast_to(
            (0.125 * weight[0, base + s]) / jnp.maximum(denom, 1.0), (HZ, BX)
        )
    factor[count] = jnp.zeros((HZ, BX), jnp.float32)
    spot = []
    for s in range(count):
        at = target[s] * cap
        for before in range(s):
            at = at + jnp.where(target[before] == target[s], 1, 0)
        spot.append(at)

    def soften(s, carry):
        pltpu.make_async_copy(tile_hbm.at[s], tile.at[s], load_sem.at[s]).wait()
        fz, fy = shift[0, base + s], shift[1, base + s]

        def row(y):
            return tile[s, :, pl.ds(y * BX, BX)]

        here = row(0)
        for j in range(HY):
            odd = row(2 * j + 1)
            ahead = row(2 * j + 2) if j < HY - 1 else odd
            thin[s, j] = here + odd + fy * (ahead - here)
            here = ahead
        for j in range(HY):
            even = thin[s, j, pl.ds(0, HZ, stride=2), :]
            odd = thin[s, j, pl.ds(1, HZ, stride=2), :]
            ahead = jnp.where(last, odd, pltpu.roll(even, HZ - 1, 0))
            top, rest = split(even + odd + fz * (ahead - even))
            place = (pl.ds((j // 2) * HZ, HZ), pl.ds((j % 2) * BX, BX))
            high[s, place[0], place[1]] = top.astype(jnp.float32)
            low[s, place[0], place[1]] = rest.astype(jnp.float32)
        return carry

    lax.fori_loop(0, count, soften, 0)

    def halve(s, carry):
        half[s] = jnp.dot(
            high[s].astype(jnp.bfloat16), matrix, preferred_element_type=jnp.float32
        ) + jnp.dot(low[s].astype(jnp.bfloat16), matrix, preferred_element_type=jnp.float32)
        return carry

    lax.fori_loop(0, count, halve, 0, unroll=True)
    half[count] = jnp.zeros((rows, 2 * BX), jnp.float32)

    for place in range(n_acq * cap):
        s = count
        for i in range(count):
            s = jnp.where(spot[i] == place, i, s)
        fx = shift[2, base + jnp.minimum(s, count - 1)]
        value = half[s, :, pl.ds(0, BX)] + fx * half[s, :, pl.ds(BX, BX)]
        scale = factor[s]
        for p in range(PAIRS):
            send[place, :, pl.ds(p * BX, BX)] = scale * value[p * HZ : (p + 1) * HZ]

    pl.semaphore_wait(barrier, n_acq - 1 + n_grp - 1)

    def to_acq(i, c):
        d, spot_at = sends[i]
        peer = flip(a, d)
        return pltpu.make_async_remote_copy(
            src_ref=send.at[peer * cap + c], dst_ref=gath.at[g, spot_at * cap + c],
            send_sem=send_a.at[0], recv_sem=recv_a.at[spot_at * cap + c],
            device_id=(peer, g), device_id_type=MESH,
        )

    def from_acq(i):
        return pltpu.make_async_remote_copy(
            src_ref=gath.at[g, i], dst_ref=gath.at[g, i],
            send_sem=send_a.at[0], recv_sem=recv_a.at[i],
            device_id=(flip(a, order[i // cap]), g), device_id_type=MESH,
        )

    def along(owner, pieces, peer, send_sem, recv_sem):
        piece = gath.at[owner, pieces]
        return pltpu.make_async_remote_copy(
            src_ref=piece, dst_ref=piece, send_sem=send_sem, recv_sem=recv_sem,
            device_id=(a, peer), device_id_type=MESH,
        )

    def over_x(owner, i, peer, d):
        return along(owner, i, peer, send_x.at[d - 1], recv_x.at[d - 1, i])

    def to_mate(owner, pieces, d, h):
        return along(owner, pieces, mate, send_c.at[d], recv_c.at[d, h])

    sends, order = layout(a, lo, n_acq)
    total = n_acq * cap
    middle = total // 2

    for c in range(cap):
        gath[g, c] = send[a * cap + c]
    for i in range(len(sends)):
        for c in range(cap):
            to_acq(i, c).start()

    others = [((hi + d) % n_hi) * 2 + lo for d in range(1, n_hi)]
    origins = [((hi + n_hi - d) % n_hi) * 2 + lo for d in range(1, n_hi)]
    mates = [((hi + n_hi - d) % n_hi) * 2 + 1 - lo for d in range(1, n_hi)]

    def forward(i):
        for d, peer in enumerate(others, 1):
            over_x(g, i, peer, d).start()
        to_mate(g, i, 0, i // middle).start()

    def relay(i):
        for d, owner in enumerate(origins, 1):
            over_x(owner, i, mate, d).wait_recv()
            to_mate(owner, i, d, i // middle).start()

    def arrived(d, h):
        owner = [mate, *mates][d]
        to_mate(owner, pl.ds(h * middle, middle), d, h).wait_recv()

    for c in range(cap):
        forward(c)

    depth = n_acq * cap * HZ
    side = depth // 2
    tall = PAR_DEV * 8 * HZ
    lane = lax.broadcasted_iota(jnp.int32, (HZ, depth), 1)
    at_slot = (lane % side) // HZ

    found = [jnp.zeros((HZ, depth), jnp.int32)] * 2
    for p, d in enumerate(order):
        first = (flip(a, d) * n_grp + g) * count
        seen = 0
        slots = [0] * cap
        for s in range(count):
            hit = jnp.where(dest[0, first + s] == a, 1, 0)
            for c in range(cap):
                slots[c] = jnp.where(
                    (hit == 1) & (seen == c), slot[0, first + s], slots[c]
                )
            seen = seen + hit
        h = p // (n_acq // 2)
        for c in range(cap):
            at = p * cap + c - h * (side // HZ)
            found[h] = jnp.where(at_slot == at, parent[0, slots[c]], found[h])
    for h in range(2):
        named[g, h] = found[h]

    def telling(d, owner, peer):
        return pltpu.make_async_remote_copy(
            src_ref=named.at[owner], dst_ref=named.at[owner],
            send_sem=send_p.at[0], recv_sem=recv_p.at[owner],
            device_id=(a, peer), device_id_type=MESH,
        )

    for d in range(1, n_grp):
        telling(d, g, (g + d) % n_grp).start()

    upright = lax.broadcasted_iota(jnp.int32, (tall, depth), 0) + g * tall
    across_lane = lax.broadcasted_iota(jnp.int32, (tall, depth), 1) % HZ

    def place_rows(owner, h):
        placing = jnp.where(
            named[owner, h, pl.ds(0, 1), :] * HZ + across_lane == upright, 1.0, 0.0
        ).astype(jnp.bfloat16)
        rows = gath[owner, pl.ds(h * (side // HZ), side // HZ)].reshape(side, LANES)
        return jnp.dot(
            placing, jnp.concatenate(split(rows), axis=0), preferred_element_type=jnp.float32
        )

    def mine():
        out[...] = place_rows(g, 0)
        for d in range(1, n_grp):
            owner = (g + n_grp - d) % n_grp
            telling(d, owner, owner).wait_recv()
        arrived(0, 0)
        out[...] += place_rows(mate, 0)

    def theirs():
        for owner in origins:
            out[...] += place_rows(owner, 0)
        for d, owner in enumerate(mates, 1):
            arrived(d, 0)
            out[...] += place_rows(owner, 0)

    def receive(start, stop):
        for i in range(start, stop):
            from_acq(i).wait_recv()
            forward(i)

    def pass_on(start, stop):
        for i in range(start, stop):
            relay(i)

    quarter = max(1, total // 4)
    eighth = max(1, total // 8)
    receive(cap, max(cap, quarter))
    for i in range(max(cap, quarter), middle):
        receive(i, i + 1)
        relay(i - max(cap, quarter))
    done = middle - max(cap, quarter)
    pass_on(done, middle - eighth)
    receive(middle, middle + eighth)
    mine()
    receive(middle + eighth, middle + quarter)
    pass_on(middle - eighth, middle)
    receive(middle + quarter, total - eighth)
    pass_on(middle, middle + eighth)
    receive(total - eighth, total)
    pass_on(middle + eighth, middle + eighth + 1)
    theirs()
    pass_on(middle + eighth + 1, total - 2)
    out[...] += place_rows(g, 1)
    pass_on(total - 2, total)
    arrived(0, 1)
    out[...] += place_rows(mate, 1)
    for owner in origins:
        out[...] += place_rows(owner, 1)
    for d, owner in enumerate(mates, 1):
        arrived(d, 1)
        out[...] += place_rows(owner, 1)

    pltpu.make_async_remote_copy(
        src_ref=send.at[pl.ds(cap, total - cap)], dst_ref=send.at[pl.ds(cap, total - cap)],
        send_sem=send_a.at[0], recv_sem=recv_a.at[0],
        device_id=(flip(a, 1), g), device_id_type=MESH,
    ).wait_send()
    pltpu.make_async_remote_copy(
        src_ref=named.at[pl.ds(1, n_grp - 1)], dst_ref=named.at[pl.ds(1, n_grp - 1)],
        send_sem=send_p.at[0], recv_sem=recv_p.at[0],
        device_id=(a, mate), device_id_type=MESH,
    ).wait_send()
    whole = pl.ds(0, total)
    for d in range(1, n_hi):
        along(g, whole, mate, send_x.at[d - 1], recv_x.at[d - 1, 0]).wait_send()
    for d in range(n_hi):
        to_mate(g, whole, d, 0).wait_send()


def body(tile_slabs, dest_rank, block_slot, shifts, blend_weight, parent_map):
    n_acq, n_grp = lax.axis_size("acq"), lax.axis_size("grp")
    count = tile_slabs.shape[0]
    subs = dest_rank.shape[0]
    blocks = parent_map.shape[0]
    cap = max(2, 2 * count // n_acq)
    depth = n_acq * cap * HZ
    hbm = pl.BlockSpec(memory_space=pltpu.HBM)
    rows = PAIRS * HZ
    dma = pltpu.SemaphoreType.DMA
    n_hi = n_grp // 2
    pieces = n_acq * cap
    summed = pl.pallas_call(
        functools.partial(kernel, n_acq, n_grp, cap),
        out_shape=pltpu.VMEM((PAR_DEV * 8 * HZ, LANES), jnp.float32),
        in_specs=[hbm] * 6,
        out_specs=pl.BlockSpec(memory_space=pltpu.VMEM),
        scratch_shapes=[
            pltpu.SMEM((1, subs), jnp.int32),
            pltpu.SMEM((1, subs), jnp.int32),
            pltpu.SMEM((1, subs), jnp.float32),
            pltpu.SMEM((3, subs), jnp.float32),
            pltpu.SMEM((1, blocks), jnp.int32),
            pltpu.VMEM((1, subs), jnp.int32),
            pltpu.VMEM((1, subs), jnp.int32),
            pltpu.VMEM((1, subs), jnp.float32),
            pltpu.VMEM((count, BZ, BY * BX), jnp.float32),
            pltpu.VMEM((count, HY, BZ, BX), jnp.float32),
            pltpu.VMEM((count, rows, 2 * BX), jnp.float32),
            pltpu.VMEM((count, rows, 2 * BX), jnp.float32),
            pltpu.VMEM((count + 1, rows, 2 * BX), jnp.float32),
            pltpu.VMEM((count + 1, HZ, BX), jnp.float32),
            pltpu.VMEM((n_acq * cap, HZ, LANES), jnp.float32),
            pltpu.VMEM((n_grp, n_acq * cap, HZ, LANES), jnp.float32),
            pltpu.VMEM((n_grp, 2, HZ, depth), jnp.int32),
            dma((8,)), dma((count,)),
            dma((1,)), dma((pieces,)),
            dma((max(1, n_hi - 1),)), dma((max(1, n_hi - 1), pieces)),
            dma((n_hi,)), dma((n_hi, 2)),
            dma((1,)), dma((n_grp,)),
        ],
        compiler_params=pltpu.CompilerParams(
            collective_id=0, has_side_effects=True, vmem_limit_bytes=VMEM_LIMIT * 2**20
        ),
    )(
        tile_slabs, dest_rank.reshape(1, subs), block_slot.reshape(1, subs),
        blend_weight.reshape(1, subs), shifts.T, parent_map.reshape(1, blocks),
    )
    return summed.reshape(PAR_DEV, 8, HZ, LANES)


def solution(mesh):
    placed = (P(("acq", "grp"), None, None), P(), P(), P(), P(), P(("acq", "grp")))
    return jax.shard_map(
        body,
        mesh=mesh,
        in_specs=placed,
        out_specs=P(("acq", "grp"), None, None, None),
        check_vma=False,
    )
```

```python
import functools
import jax
import jax.numpy as jnp
from jax import lax
from jax.experimental import pallas as pl
from jax.experimental.pallas import tpu as pltpu
from jax.sharding import PartitionSpec as P

BZ = 16
BY = 32
BX = 128
PAR_DEV = 2
HZ, HY, HX = BZ // 2, BY // 2, BX // 2
PAIRS = HY // 2
LANES = HY * HX
PER_LOAD = 2
VMEM_LIMIT = 62
MESH = pl.DeviceIdType.MESH


def flip(index, mask):
    out, bit = index, 1
    while bit < 64:
        out = out + bit * ((mask // bit) % 2) * (1 - 2 * ((index // bit) % 2))
        bit *= 2
    return out


def orders(count):
    unit = count // 4
    if unit < 1:
        plain = list(range(1, count))
        return plain, [[0] + plain] * 4
    half = unit - unit // 2
    side, near, far, farther = [list(range(q * unit, (q + 1) * unit)) for q in range(4)]
    side = side[1:]
    sends = side + near + far + farther
    arrivals = [
        [0] + side + far[:half] + near + farther[:half] + far[half:] + farther[half:],
        [0] + sends,
        [0] + far[:half] + side + far[half:] + near + farther,
        [0] + side + near + farther[:half] + far + farther[half:],
    ]
    return sends, arrivals


def layout(index, lo, count):
    sends, arrivals = orders(count)
    unit = max(1, count // 4)
    row = index // unit
    inner = (row + row // 2) % 2 if count >= 4 else 0

    def pick(*cases):
        if len(cases) == 2:
            return cases[0] + inner * (cases[1] - cases[0])
        below, above = pick(*cases[:2]), pick(*cases[2:])
        return below + lo * (above - below)

    def landing(d, within, low):
        if (d // unit) % 4 in (1, 2):
            within = 1 - within
        return arrivals[2 * low + within].index(d)

    targets = [
        (d, pick(*[landing(d, within, low) for low in range(2) for within in range(2)]))
        for d in sends
    ]
    return targets, [pick(*cases) for cases in zip(*arrivals)]


def halving_matrix():
    row = lax.broadcasted_iota(jnp.int32, (2 * BX, 2 * BX), 0)
    col = lax.broadcasted_iota(jnp.int32, (2 * BX, 2 * BX), 1)
    x, y = row % BX, row // BX
    cx, cy, part = col % HX, (col // HX) % 2, col // BX
    same = y == cy
    both = jnp.where(same & (x // 2 == cx), 1.0, 0.0)
    ahead = jnp.where(same & (x == jnp.minimum(2 * cx + 2, BX - 1)), 1.0, 0.0)
    here = jnp.where(same & (x == 2 * cx), 1.0, 0.0)
    return jnp.where(part == 0, both, ahead - here).astype(jnp.bfloat16)


def split(values):
    high = values.astype(jnp.bfloat16)
    return high, (values - high.astype(jnp.float32)).astype(jnp.bfloat16)


def kernel(
    n_acq, n_grp, cap, tile_hbm, dest_hbm, slot_hbm, weight_hbm, shift_hbm, parent_hbm, out,
    named_by, weight, shift, parent, named_rows, weight_row,
    tile, thin, high, low, half, factor, send, gath, named,
    meta_sem, load_sem, send_a, recv_a, send_x, recv_x, send_c, recv_c, send_p, recv_p,
):
    count = tile.shape[0]
    a, g = lax.axis_index("acq"), lax.axis_index("grp")
    hi, lo = g // 2, g % 2
    mate = hi * 2 + (1 - lo)
    n_hi = n_grp // 2
    rows = PAIRS * HZ

    barrier = pltpu.get_barrier_semaphore()
    for d in range(1, n_acq):
        pl.semaphore_signal(barrier, inc=1, device_id=((a + d) % n_acq, g), device_id_type=MESH)
    for d in range(1, n_grp):
        pl.semaphore_signal(barrier, inc=1, device_id=(a, (g + d) % n_grp), device_id_type=MESH)

    dest, slot = named_by.at[0], named_by.at[1]
    metas = [
        pltpu.make_async_copy(start, end, meta_sem.at[i])
        for start, end, i in (
            (dest_hbm, dest, 0), (slot_hbm, slot, 0), (weight_hbm, weight, 1),
            (shift_hbm, shift, 2), (parent_hbm, parent, 3),
            (dest_hbm, named_rows.at[0], 4), (slot_hbm, named_rows.at[1], 4),
            (weight_hbm, weight_row, 5),
        )
    ]
    for meta in metas:
        meta.start()

    def load(i):
        some = pl.ds(i * PER_LOAD, PER_LOAD)
        return pltpu.make_async_copy(tile_hbm.at[some], tile.at[some], load_sem.at[i])

    for i in range(count // PER_LOAD):
        load(i).start()

    matrix = halving_matrix()
    last = lax.broadcasted_iota(jnp.int32, (HZ, BX), 0) == HZ - 1
    for pair, i in ((named_by, 0), (named_rows, 4)):
        pltpu.make_async_copy(pair, pair, meta_sem.at[i]).wait()
    for i in (2, 3, 4, 7):
        metas[i].wait()

    blocks = parent.shape[1]
    base = (a * n_grp + g) * count
    target = [dest[0, base + s] for s in range(count)]
    key = [target[s] * blocks + slot[0, base + s] for s in range(count)]
    subs = lax.broadcasted_iota(jnp.int32, weight_row.shape, 1)
    keys = jnp.where(
        (subs // count) % n_grp == g, named_rows[0] * blocks + named_rows[1], -1
    )
    for s in range(count):
        denom = jnp.sum(jnp.where(keys == key[s], weight_row[...], 0.0), axis=1, keepdims=True)
        factor[s] = jnp.broadcast_to(
            (0.125 * weight[0, base + s]) / jnp.maximum(denom, 1.0), (HZ, BX)
        )
    factor[count] = jnp.zeros((HZ, BX), jnp.float32)
    spot = []
    for s in range(count):
        at = target[s] * cap
        for before in range(s):
            at = at + jnp.where(target[before] == target[s], 1, 0)
        spot.append(at)

    def soften(s):
        fz, fy = shift[0, base + s], shift[1, base + s]

        def row(y):
            return tile[s, :, pl.ds(y * BX, BX)]

        here = row(0)
        for j in range(HY):
            odd = row(2 * j + 1)
            ahead = row(2 * j + 2) if j < HY - 1 else odd
            thin[s, j] = here + odd + fy * (ahead - here)
            here = ahead
        for j in range(HY):
            even = thin[s, j, pl.ds(0, HZ, stride=2), :]
            odd = thin[s, j, pl.ds(1, HZ, stride=2), :]
            ahead = jnp.where(last, odd, pltpu.roll(even, HZ - 1, 0))
            top, rest = split(even + odd + fz * (ahead - even))
            place = (pl.ds((j // 2) * HZ, HZ), pl.ds((j % 2) * BX, BX))
            high[s, place[0], place[1]] = top.astype(jnp.float32)
            low[s, place[0], place[1]] = rest.astype(jnp.float32)

    def loaded(i, carry):
        load(i).wait()
        for s in range(PER_LOAD):
            soften(i * PER_LOAD + s)
        return carry

    lax.fori_loop(0, count // PER_LOAD, loaded, 0)

    def halve(s, carry):
        half[s] = jnp.dot(
            high[s].astype(jnp.bfloat16), matrix, preferred_element_type=jnp.float32
        ) + jnp.dot(low[s].astype(jnp.bfloat16), matrix, preferred_element_type=jnp.float32)
        return carry

    lax.fori_loop(0, count, halve, 0, unroll=True)
    half[count] = jnp.zeros((rows, 2 * BX), jnp.float32)

    for place in range(n_acq * cap):
        s = count
        for i in range(count):
            s = jnp.where(spot[i] == place, i, s)
        fx = shift[2, base + jnp.minimum(s, count - 1)]
        value = half[s, :, pl.ds(0, BX)] + fx * half[s, :, pl.ds(BX, BX)]
        scale = factor[s]
        for p in range(PAIRS):
            send[place, :, pl.ds(p * BX, BX)] = scale * value[p * HZ : (p + 1) * HZ]

    pl.semaphore_wait(barrier, n_acq - 1 + n_grp - 1)

    targets, order = layout(a, lo, n_acq)
    total = n_acq * cap
    middle = total // 2
    direct = total - cap
    received = [(i, cap) for i in range(cap, middle, cap)] + [(i, 1) for i in range(middle, total)]
    groups, first = [], 0
    while first < total:
        size = max(1, (total - first) // 2)
        groups.append((first, size))
        first += size

    def landed(at, c):
        late = at // (n_acq // 2)
        return recv_a.at[at + late * ((at - n_acq // 2) * (cap - 1) + c)]

    def to_acq(d, at, c):
        peer = flip(a, d)
        return pltpu.make_async_remote_copy(
            src_ref=send.at[peer * cap + c], dst_ref=gath.at[g, at * cap + c],
            send_sem=send_a.at[0], recv_sem=landed(at, c),
            device_id=(peer, g), device_id_type=MESH,
        )

    def from_acq(i, size):
        piece = gath.at[g, pl.ds(i, size)]
        return pltpu.make_async_remote_copy(
            src_ref=piece, dst_ref=piece,
            send_sem=send_a.at[0], recv_sem=landed(i // cap, i % cap),
            device_id=(flip(a, order[i // cap]), g), device_id_type=MESH,
        )

    def along(owner, first, size, peer, send_sem, recv_sem):
        piece = gath.at[owner, pl.ds(first, size)]
        return pltpu.make_async_remote_copy(
            src_ref=piece, dst_ref=piece, send_sem=send_sem, recv_sem=recv_sem,
            device_id=(a, peer), device_id_type=MESH,
        )

    others = [((hi + d) % n_hi) * 2 + lo for d in range(1, n_hi)]
    origins = [((hi + n_hi - d) % n_hi) * 2 + lo for d in range(1, n_hi)]
    mates = [((hi + n_hi - d) % n_hi) * 2 + 1 - lo for d in range(1, n_hi)]

    def over_x(owner, first, size, peer, d):
        k = max(k for k, (start, _) in enumerate(groups) if start <= first)
        return along(owner, first, size, peer, send_x.at[d - 1], recv_x.at[d - 1, k])

    def aside(first, size, peer, d):
        return along(g, first, size, peer, send_x.at[d - 1], recv_c.at[d, 1])

    def to_mate(owner, first, size, d):
        return along(owner, first, size, mate, send_c.at[d], recv_c.at[d, first // middle])

    def forward(i, size):
        for d, peer in enumerate(others, 1):
            over_x(g, i, size, peer, d).start()
            if i >= direct:
                @pl.when(lo == 0)
                def _():
                    aside(i, size, (peer // 2) * 2 + 1, d).start()
        to_mate(g, i, size, 0).start()

    def relay(first, size):
        for d, owner in enumerate(origins, 1):
            over_x(owner, first, size, mate, d).wait_recv()
            if first < direct:
                to_mate(owner, first, size, d).start()
            else:
                @pl.when(lo == 1)
                def _():
                    to_mate(owner, first, size, d).start()

    def arrived(d, h):
        to_mate([mate, *mates][d], h * middle, middle, d).wait_recv()

    for c in range(cap):
        gath[g, c] = send[a * cap + c]
    for d, at in targets:
        for c in range(cap):
            to_acq(d, at, c).start()
    forward(0, cap)

    depth = n_acq * cap * HZ
    side = depth // 2
    tall = PAR_DEV * 8 * HZ
    lane = lax.broadcasted_iota(jnp.int32, (HZ, depth), 1)
    at_slot = (lane % side) // HZ

    found = [jnp.zeros((HZ, depth), jnp.int32)] * 2
    for p, d in enumerate(order):
        first = (flip(a, d) * n_grp + g) * count
        seen = 0
        slots = [0] * cap
        for s in range(count):
            hit = jnp.where(dest[0, first + s] == a, 1, 0)
            for c in range(cap):
                slots[c] = jnp.where(
                    (hit == 1) & (seen == c), slot[0, first + s], slots[c]
                )
            seen = seen + hit
        h = p // (n_acq // 2)
        for c in range(cap):
            at = p * cap + c - h * (side // HZ)
            found[h] = jnp.where(at_slot == at, parent[0, slots[c]], found[h])
    for h in range(2):
        named[0, h] = found[h]

    def telling(d, peer):
        return pltpu.make_async_remote_copy(
            src_ref=named.at[0], dst_ref=named.at[d],
            send_sem=send_p.at[0], recv_sem=recv_p.at[0],
            device_id=(a, peer), device_id_type=MESH,
        )

    for d in range(1, n_grp):
        telling(d, (g + d) % n_grp).start()

    upright = lax.broadcasted_iota(jnp.int32, (tall, depth), 0) + g * tall
    across_lane = lax.broadcasted_iota(jnp.int32, (tall, depth), 1) % HZ

    def place_rows(owner, h):
        placing = jnp.where(
            named[(g + n_grp - owner) % n_grp, h, pl.ds(0, 1), :] * HZ + across_lane == upright, 1.0, 0.0
        ).astype(jnp.bfloat16)
        rows = gath[owner, pl.ds(h * (side // HZ), side // HZ)].reshape(side, LANES)
        return jnp.dot(
            placing, jnp.concatenate(split(rows), axis=0), preferred_element_type=jnp.float32
        )

    for i, size in received:
        from_acq(i, size).wait_recv()
        forward(i, size)
    out[...] = place_rows(g, 0)
    out[...] += place_rows(g, 1)
    relay(*groups[0])
    others_named = named.at[pl.ds(1, n_grp - 1)]
    naming = pltpu.make_async_remote_copy(
        src_ref=others_named, dst_ref=others_named,
        send_sem=send_p.at[0], recv_sem=recv_p.at[0],
        device_id=(a, mate), device_id_type=MESH,
    )
    naming.wait_recv()
    for owner in origins:
        out[...] += place_rows(owner, 0)
    for k in range(1, len(groups)):
        relay(*groups[k])
        if k == 1:
            arrived(0, 0)
            out[...] += place_rows(mate, 0)
    arrived(0, 1)
    out[...] += place_rows(mate, 1)
    for d, owner in enumerate(mates, 1):
        arrived(d, 0)
        out[...] += place_rows(owner, 0)
    for owner in origins:
        out[...] += place_rows(owner, 1)
    for d, owner in enumerate(mates, 1):
        arrived(d, 1)
        out[...] += place_rows(owner, 1)

    naming.wait_send()
    left = send.at[pl.ds(cap, total - cap)]
    pltpu.make_async_remote_copy(
        src_ref=left, dst_ref=left, send_sem=send_a.at[0], recv_sem=recv_a.at[0],
        device_id=(flip(a, 1), g), device_id_type=MESH,
    ).wait_send()
    to_mate(g, 0, total, 0).wait_send()
    for d in range(1, n_hi):
        over_x(g, 0, total, mate, d).wait_send()
        to_mate(g, 0, direct, d).wait_send()

        @pl.when(lo == 0)
        def _():
            aside(direct, total - direct, mate, d).wait_send()

        @pl.when(lo == 1)
        def _():
            to_mate(g, direct, total - direct, d).wait_send()


def body(tile_slabs, dest_rank, block_slot, shifts, blend_weight, parent_map):
    n_acq, n_grp = lax.axis_size("acq"), lax.axis_size("grp")
    count = tile_slabs.shape[0]
    subs = dest_rank.shape[0]
    blocks = parent_map.shape[0]
    cap = max(2, 2 * count // n_acq)
    depth = n_acq * cap * HZ
    hbm = pl.BlockSpec(memory_space=pltpu.HBM)
    rows = PAIRS * HZ
    dma = pltpu.SemaphoreType.DMA
    n_hi = n_grp // 2
    pieces = n_acq * cap
    summed = pl.pallas_call(
        functools.partial(kernel, n_acq, n_grp, cap),
        out_shape=pltpu.VMEM((PAR_DEV * 8 * HZ, LANES), jnp.float32),
        in_specs=[hbm] * 6,
        out_specs=pl.BlockSpec(memory_space=pltpu.VMEM),
        scratch_shapes=[
            pltpu.SMEM((2, 1, subs), jnp.int32),
            pltpu.SMEM((1, subs), jnp.float32),
            pltpu.SMEM((3, subs), jnp.float32),
            pltpu.SMEM((1, blocks), jnp.int32),
            pltpu.VMEM((2, 1, subs), jnp.int32),
            pltpu.VMEM((1, subs), jnp.float32),
            pltpu.VMEM((count, BZ, BY * BX), jnp.float32),
            pltpu.VMEM((count, HY, BZ, BX), jnp.float32),
            pltpu.VMEM((count, rows, 2 * BX), jnp.float32),
            pltpu.VMEM((count, rows, 2 * BX), jnp.float32),
            pltpu.VMEM((count + 1, rows, 2 * BX), jnp.float32),
            pltpu.VMEM((count + 1, HZ, BX), jnp.float32),
            pltpu.VMEM((n_acq * cap, HZ, LANES), jnp.float32),
            pltpu.VMEM((n_grp, n_acq * cap, HZ, LANES), jnp.float32),
            pltpu.VMEM((n_grp, 2, HZ, depth), jnp.int32),
            dma((6,)), dma((count // PER_LOAD,)),
            dma((1,)), dma((n_acq // 2 * (1 + cap),)),
            dma((max(1, n_hi - 1),)), dma((max(1, n_hi - 1), pieces.bit_length())),
            dma((n_hi,)), dma((n_hi, 2)),
            dma((1,)), dma((1,)),
        ],
        compiler_params=pltpu.CompilerParams(
            collective_id=0, has_side_effects=True, vmem_limit_bytes=VMEM_LIMIT * 2**20
        ),
    )(
        tile_slabs, dest_rank.reshape(1, subs), block_slot.reshape(1, subs),
        blend_weight.reshape(1, subs), shifts.T, parent_map.reshape(1, blocks),
    )
    return summed.reshape(PAR_DEV, 8, HZ, LANES)


def solution(mesh):
    placed = (P(("acq", "grp"), None, None), P(), P(), P(), P(), P(("acq", "grp")))
    return jax.shard_map(
        body,
        mesh=mesh,
        in_specs=placed,
        out_specs=P(("acq", "grp"), None, None, None),
        check_vma=False,
    )
```

```python
import functools
import jax
import jax.numpy as jnp
from jax import lax
from jax.experimental import pallas as pl
from jax.experimental.pallas import tpu as pltpu
from jax.sharding import PartitionSpec as P

BZ = 16
BY = 32
BX = 128
PAR_DEV = 2
HZ, HY, HX = BZ // 2, BY // 2, BX // 2
PAIRS = HY // 2
LANES = HY * HX
PER_LOAD = 2
VMEM_LIMIT = 62
MESH = pl.DeviceIdType.MESH


def flip(index, mask):
    out, bit = index, 1
    while bit < 64:
        out = out + bit * ((mask // bit) % 2) * (1 - 2 * ((index // bit) % 2))
        bit *= 2
    return out


def orders(count):
    unit = count // 4
    if unit < 1:
        plain = list(range(1, count))
        return plain, [[0] + plain] * 4
    half = unit - unit // 2
    side, near, far, farther = [list(range(q * unit, (q + 1) * unit)) for q in range(4)]
    side = side[1:]
    sends = side + near + far + farther
    arrivals = [
        [0] + side + far[:half] + near + far[half:] + farther,
        [0] + sends,
        [0] + far[:half] + side + far[half:] + near + farther,
        [0] + side + near + farther[:half] + far + farther[half:],
    ]
    return sends, arrivals


def layout(index, lo, count):
    sends, arrivals = orders(count)
    unit = max(1, count // 4)
    row = index // unit
    inner = (row + row // 2) % 2 if count >= 4 else 0

    def pick(*cases):
        if len(cases) == 2:
            return cases[0] + inner * (cases[1] - cases[0])
        below, above = pick(*cases[:2]), pick(*cases[2:])
        return below + lo * (above - below)

    def landing(d, within, low):
        if (d // unit) % 4 in (1, 2):
            within = 1 - within
        return arrivals[2 * low + within].index(d)

    targets = [
        (d, pick(*[landing(d, within, low) for low in range(2) for within in range(2)]))
        for d in sends
    ]
    return targets, [pick(*cases) for cases in zip(*arrivals)]


def halving_matrix():
    row = lax.broadcasted_iota(jnp.int32, (2 * BX, 2 * BX), 0)
    col = lax.broadcasted_iota(jnp.int32, (2 * BX, 2 * BX), 1)
    x, y = row % BX, row // BX
    cx, cy, part = col % HX, (col // HX) % 2, col // BX
    same = y == cy
    both = jnp.where(same & (x // 2 == cx), 1.0, 0.0)
    ahead = jnp.where(same & (x == jnp.minimum(2 * cx + 2, BX - 1)), 1.0, 0.0)
    here = jnp.where(same & (x == 2 * cx), 1.0, 0.0)
    return jnp.where(part == 0, both, ahead - here).astype(jnp.bfloat16)


def split(values):
    high = values.astype(jnp.bfloat16)
    return high, (values - high.astype(jnp.float32)).astype(jnp.bfloat16)


def kernel(
    n_acq, n_grp, cap, tile_hbm, dest_hbm, slot_hbm, weight_hbm, shift_hbm, parent_hbm, out,
    named_by, weight, shift, parent, named_rows, weight_row,
    tile, thin, high, low, half, factor, send, gath, named,
    meta_sem, load_sem, send_a, recv_a, send_x, recv_x, send_c, recv_c, send_p, recv_p, recv_r, recv_s,
):
    count = tile.shape[0]
    a, g = lax.axis_index("acq"), lax.axis_index("grp")
    hi, lo = g // 2, g % 2
    mate = hi * 2 + (1 - lo)
    n_hi = n_grp // 2
    rows = PAIRS * HZ

    barrier = pltpu.get_barrier_semaphore()
    for d in range(1, n_acq):
        pl.semaphore_signal(barrier, inc=1, device_id=((a + d) % n_acq, g), device_id_type=MESH)
    for d in range(1, n_grp):
        pl.semaphore_signal(barrier, inc=1, device_id=(a, (g + d) % n_grp), device_id_type=MESH)
    lent = n_acq // 4 + n_acq // 8
    for d in range(n_acq - lent, n_acq):
        @pl.when(lo == 1)
        def _():
            pl.semaphore_signal(barrier, inc=1, device_id=(flip(a, d), mate), device_id_type=MESH)

    dest, slot = named_by.at[0], named_by.at[1]
    metas = [
        pltpu.make_async_copy(start, end, meta_sem.at[i])
        for start, end, i in (
            (dest_hbm, dest, 0), (slot_hbm, slot, 0), (weight_hbm, weight, 1),
            (shift_hbm, shift, 2), (parent_hbm, parent, 3),
            (dest_hbm, named_rows.at[0], 4), (slot_hbm, named_rows.at[1], 4),
            (weight_hbm, weight_row, 5),
        )
    ]
    for meta in metas:
        meta.start()

    def load(i):
        some = pl.ds(i * PER_LOAD, PER_LOAD)
        return pltpu.make_async_copy(tile_hbm.at[some], tile.at[some], load_sem.at[i])

    for i in range(count // PER_LOAD):
        load(i).start()

    matrix = halving_matrix()
    last = lax.broadcasted_iota(jnp.int32, (HZ, BX), 0) == HZ - 1
    for pair, i in ((named_by, 0), (named_rows, 4)):
        pltpu.make_async_copy(pair, pair, meta_sem.at[i]).wait()
    for i in (2, 3, 4, 7):
        metas[i].wait()

    blocks = parent.shape[1]
    base = (a * n_grp + g) * count
    target = [dest[0, base + s] for s in range(count)]
    key = [target[s] * blocks + slot[0, base + s] for s in range(count)]
    subs = lax.broadcasted_iota(jnp.int32, weight_row.shape, 1)
    keys = jnp.where(
        (subs // count) % n_grp == g, named_rows[0] * blocks + named_rows[1], -1
    )
    for s in range(count):
        denom = jnp.sum(jnp.where(keys == key[s], weight_row[...], 0.0), axis=1, keepdims=True)
        factor[s] = jnp.broadcast_to(
            (0.125 * weight[0, base + s]) / jnp.maximum(denom, 1.0), (HZ, BX)
        )
    factor[count] = jnp.zeros((HZ, BX), jnp.float32)
    spot = []
    for s in range(count):
        at = target[s] * cap
        for before in range(s):
            at = at + jnp.where(target[before] == target[s], 1, 0)
        spot.append(at)

    chosen = []
    for place in range(n_acq * cap):
        s = count
        for i in range(count):
            s = jnp.where(spot[i] == place, i, s)
        chosen.append(s)

    def soften(s):
        fz, fy = shift[0, base + s], shift[1, base + s]

        def row(y):
            return tile[s, :, pl.ds(y * BX, BX)]

        here = row(0)
        for j in range(HY):
            odd = row(2 * j + 1)
            ahead = row(2 * j + 2) if j < HY - 1 else odd
            thin[s, j] = here + odd + fy * (ahead - here)
            here = ahead
        for j in range(HY):
            even = thin[s, j, pl.ds(0, HZ, stride=2), :]
            odd = thin[s, j, pl.ds(1, HZ, stride=2), :]
            ahead = jnp.where(last, odd, pltpu.roll(even, HZ - 1, 0))
            top, rest = split(even + odd + fz * (ahead - even))
            place = (pl.ds((j // 2) * HZ, HZ), pl.ds((j % 2) * BX, BX))
            high[s, place[0], place[1]] = top.astype(jnp.float32)
            low[s, place[0], place[1]] = rest.astype(jnp.float32)

    def halve(s):
        half[s] = jnp.dot(
            high[s].astype(jnp.bfloat16), matrix, preferred_element_type=jnp.float32
        ) + jnp.dot(low[s].astype(jnp.bfloat16), matrix, preferred_element_type=jnp.float32)

    def loaded(i, carry):
        load(i).wait()
        for s in range(PER_LOAD):
            soften(i * PER_LOAD + s)
        return carry

    lax.fori_loop(0, count // PER_LOAD, loaded, 0)
    for s in range(count):
        halve(s)

    half[count] = jnp.zeros((rows, 2 * BX), jnp.float32)

    for place in range(n_acq * cap):
        s = chosen[place]
        fx = shift[2, base + jnp.minimum(s, count - 1)]
        value = half[s, :, pl.ds(0, BX)] + fx * half[s, :, pl.ds(BX, BX)]
        scale = factor[s]
        for p in range(PAIRS):
            send[place, :, pl.ds(p * BX, BX)] = scale * value[p * HZ : (p + 1) * HZ]

    pl.semaphore_wait(barrier, n_acq - 1 + n_grp - 1 + lent * (1 - lo))

    targets, order = layout(a, lo, n_acq)
    total = n_acq * cap
    middle = total // 2
    shared = total - lent * cap
    received = [(i, cap) for i in range(cap, middle, cap)] + [(i, 1) for i in range(middle, shared)]
    groups, first = [(0, shared)], shared
    while first < total:
        size = max(1, total - cap - first)
        groups.append((first, size))
        first += size
    halved = list(range(shared + (total - shared) // 3, total - cap))
    borrowed = (
        list(range(shared, shared + (total - shared) // 3, 2)) + halved
        + list(range(shared + 1, shared + (total - shared) // 3, 2)) + list(range(total - cap, total))
    )

    def landed(at, c):
        late = at // (n_acq // 2)
        return at + late * ((at - n_acq // 2) * (cap - 1) + c)

    def lent_at(i):
        return n_acq // 2 * (1 + cap) + i - shared

    def to_acq(d, at, c):
        sem, core = landed(at, c), g
        if d >= n_acq - lent:
            sem = lo * sem + (1 - lo) * lent_at(d * cap + c)
            core = g + 1 - lo
        peer = flip(a, d)
        return pltpu.make_async_remote_copy(
            src_ref=send.at[peer * cap + c], dst_ref=gath.at[g, at * cap + c],
            send_sem=send_a.at[0], recv_sem=recv_a.at[sem],
            device_id=(peer, core), device_id_type=MESH,
        )

    def from_acq(owner, i, size, sem):
        piece = gath.at[owner, pl.ds(i, size)]
        return pltpu.make_async_remote_copy(
            src_ref=piece, dst_ref=piece, send_sem=send_a.at[0], recv_sem=recv_a.at[sem],
            device_id=(flip(a, 1), g), device_id_type=MESH,
        )

    def along(owner, first, size, peer, send_sem, recv_sem):
        piece = gath.at[owner, pl.ds(first, size)]
        return pltpu.make_async_remote_copy(
            src_ref=piece, dst_ref=piece, send_sem=send_sem, recv_sem=recv_sem,
            device_id=(a, peer), device_id_type=MESH,
        )

    others = [((hi + d) % n_hi) * 2 + lo for d in range(1, n_hi)]
    origins = [((hi + n_hi - d) % n_hi) * 2 + lo for d in range(1, n_hi)]
    mates = [((hi + n_hi - d) % n_hi) * 2 + 1 - lo for d in range(1, n_hi)]

    def over_x(owner, first, size, peer, d):
        k = max(k for k, (start, _) in enumerate(groups) if start <= first)
        return along(owner, first, size, peer, send_x.at[d - 1], recv_x.at[d - 1, k])

    def to_mate(owner, first, size, d):
        return along(owner, first, size, mate, send_c.at[d], recv_c.at[d, first // middle])

    def take(i, size):
        from_acq(g, i, size, landed(i // cap, i % cap)).wait_recv()
        for d, peer in enumerate(others, 1):
            over_x(g, i, size, peer, d).start()
        to_mate(g, i, size, 0).start()

    def lent_x(owner, i, peer, d):
        return along(owner, i, 1, peer, send_x.at[d - 1], recv_r.at[d - 1, i - shared])

    def lent_back(owner, first, size, d):
        return along(owner, first, size, mate, send_c.at[d], recv_s.at[d])

    def take_lent(i):
        from_acq(mate, i, 1, lent_at(i)).wait_recv()
        for d, peer in enumerate(others, 1):
            lent_x(mate, i, peer, d).start()
        lent_back(mate, i, 1, 0).start()

    def relay(first, size):
        for d, owner in enumerate(origins, 1):
            over_x(owner, first, size, mate, d).wait_recv()
            cut = min(max(middle - first, 0), size)
            for at, length in ((first, cut), (first + cut, size - cut)):
                if length:
                    to_mate(owner, at, length, d).start()

    def relay_lent(i):
        for d, owner in enumerate(mates, 1):
            lent_x(owner, i, mate, d).wait_recv()
            lent_back(owner, i, 1, d).start()

    def arrived(d, h):
        owner = [mate, *mates][d]
        if h == 0:
            to_mate(owner, 0, middle, d).wait_recv()
            return

        @pl.when(lo == 0)
        def _():
            to_mate(owner, middle, total - middle, d).wait_recv()

        @pl.when(lo == 1)
        def _():
            to_mate(owner, middle, shared - middle, d).wait_recv()

    for c in range(cap):
        gath[g, c] = send[a * cap + c]
    for d, at in targets:
        for c in range(cap):
            to_acq(d, at, c).start()
    for d, peer in enumerate(others, 1):
        over_x(g, 0, cap, peer, d).start()
    to_mate(g, 0, cap, 0).start()

    depth = n_acq * cap * HZ
    side = depth // 2
    tall = PAR_DEV * 8 * HZ
    lane = lax.broadcasted_iota(jnp.int32, (HZ, depth), 1)
    at_slot = (lane % side) // HZ

    found = [jnp.zeros((HZ, depth), jnp.int32)] * 2
    for p, d in enumerate(order):
        first = (flip(a, d) * n_grp + g) * count
        seen = 0
        slots = [0] * cap
        for s in range(count):
            hit = jnp.where(dest[0, first + s] == a, 1, 0)
            for c in range(cap):
                slots[c] = jnp.where(
                    (hit == 1) & (seen == c), slot[0, first + s], slots[c]
                )
            seen = seen + hit
        h = p // (n_acq // 2)
        for c in range(cap):
            at = p * cap + c - h * (side // HZ)
            found[h] = jnp.where(at_slot == at, parent[0, slots[c]], found[h])
    for h in range(2):
        named[0, h] = found[h]

    def telling(d, peer):
        return pltpu.make_async_remote_copy(
            src_ref=named.at[0], dst_ref=named.at[d],
            send_sem=send_p.at[0], recv_sem=recv_p.at[0],
            device_id=(a, peer), device_id_type=MESH,
        )

    for d in range(1, n_grp):
        telling(d, (g + d) % n_grp).start()

    upright = lax.broadcasted_iota(jnp.int32, (tall, depth), 0) + g * tall
    across_lane = lax.broadcasted_iota(jnp.int32, (tall, depth), 1) % HZ

    def place_rows(owner, h):
        placing = jnp.where(
            named[(g + n_grp - owner) % n_grp, h, pl.ds(0, 1), :] * HZ + across_lane == upright, 1.0, 0.0
        ).astype(jnp.bfloat16)
        rows = gath[owner, pl.ds(h * (side // HZ), side // HZ)].reshape(side, LANES)
        return jnp.dot(
            placing, jnp.concatenate(split(rows), axis=0), preferred_element_type=jnp.float32
        )

    for i, size in received:
        take(i, size)

    @pl.when(lo == 1)
    def _():
        for i in range(shared, total - cap):
            take(i, 1)
        waiting = list(borrowed)
        for i in range(total - cap, total):
            for _ in range(max(1, (len(borrowed) - cap) // 2 - cap // 2 + (i == total - cap))):
                take_lent(waiting.pop(0))
            take(i, 1)
        for j in waiting:
            take_lent(j)

    relay(*groups[0])

    @pl.when(lo == 1)
    def _():
        relay(*groups[1])
        relay_lent(borrowed[0])

    others_named = named.at[pl.ds(1, n_grp - 1)]
    naming = pltpu.make_async_remote_copy(
        src_ref=others_named, dst_ref=others_named,
        send_sem=send_p.at[0], recv_sem=recv_p.at[0],
        device_id=(a, mate), device_id_type=MESH,
    )
    naming.wait_recv()
    out[...] = place_rows(g, 0)
    for owner in origins:
        out[...] += place_rows(owner, 0)
    arrived(0, 0)
    out[...] += place_rows(mate, 0)

    @pl.when(lo == 0)
    def _():
        lent_back(g, shared, total - shared, 0).wait_recv()

    out[...] += place_rows(g, 1)
    arrived(0, 1)
    out[...] += place_rows(mate, 1)
    for d, owner in enumerate(mates, 1):
        arrived(d, 0)
        out[...] += place_rows(owner, 0)

    @pl.when(lo == 1)
    def _():
        rest = borrowed[1:]
        for group in groups[2:]:
            relay(*group)
            if rest:
                relay_lent(rest.pop(0))
        for i in rest:
            relay_lent(i)

    for d, owner in enumerate(mates, 1):
        arrived(d, 1)
        out[...] += place_rows(owner, 1)

    @pl.when(lo == 0)
    def _():
        for d, owner in enumerate(origins, 1):
            lent_back(owner, shared, total - shared, d).wait_recv()

    for owner in origins:
        out[...] += place_rows(owner, 1)

    naming.wait_send()
    left = send.at[pl.ds(cap, total - cap)]
    pltpu.make_async_remote_copy(
        src_ref=left, dst_ref=left, send_sem=send_a.at[0], recv_sem=recv_a.at[0],
        device_id=(flip(a, 1), g), device_id_type=MESH,
    ).wait_send()
    sent = [send_x.at[d - 1] for d in range(1, n_hi)] + [send_c.at[d] for d in range(n_hi)]
    for sem in sent:
        along(g, 0, shared, mate, sem, recv_s.at[0]).wait_send()

    @pl.when(lo == 1)
    def _():
        for sem in sent:
            for _ in range(2):
                along(g, shared, total - shared, mate, sem, recv_s.at[0]).wait_send()


def body(tile_slabs, dest_rank, block_slot, shifts, blend_weight, parent_map):
    n_acq, n_grp = lax.axis_size("acq"), lax.axis_size("grp")
    count = tile_slabs.shape[0]
    subs = dest_rank.shape[0]
    blocks = parent_map.shape[0]
    cap = max(2, 2 * count // n_acq)
    depth = n_acq * cap * HZ
    hbm = pl.BlockSpec(memory_space=pltpu.HBM)
    rows = PAIRS * HZ
    dma = pltpu.SemaphoreType.DMA
    n_hi = n_grp // 2
    pieces = n_acq * cap
    summed = pl.pallas_call(
        functools.partial(kernel, n_acq, n_grp, cap),
        out_shape=pltpu.VMEM((PAR_DEV * 8 * HZ, LANES), jnp.float32),
        in_specs=[hbm] * 6,
        out_specs=pl.BlockSpec(memory_space=pltpu.VMEM),
        scratch_shapes=[
            pltpu.SMEM((2, 1, subs), jnp.int32),
            pltpu.SMEM((1, subs), jnp.float32),
            pltpu.SMEM((3, subs), jnp.float32),
            pltpu.SMEM((1, blocks), jnp.int32),
            pltpu.VMEM((2, 1, subs), jnp.int32),
            pltpu.VMEM((1, subs), jnp.float32),
            pltpu.VMEM((count, BZ, BY * BX), jnp.float32),
            pltpu.VMEM((count, HY, BZ, BX), jnp.float32),
            pltpu.VMEM((count, rows, 2 * BX), jnp.float32),
            pltpu.VMEM((count, rows, 2 * BX), jnp.float32),
            pltpu.VMEM((count + 1, rows, 2 * BX), jnp.float32),
            pltpu.VMEM((count + 1, HZ, BX), jnp.float32),
            pltpu.VMEM((n_acq * cap, HZ, LANES), jnp.float32),
            pltpu.VMEM((n_grp, n_acq * cap, HZ, LANES), jnp.float32),
            pltpu.VMEM((n_grp, 2, HZ, depth), jnp.int32),
            dma((6,)), dma((count // PER_LOAD,)),
            dma((1,)), dma((n_acq // 2 * (1 + cap) + (n_acq // 4 + n_acq // 8) * cap,)),
            dma((max(1, n_hi - 1),)), dma((max(1, n_hi - 1), pieces.bit_length())),
            dma((n_hi,)), dma((n_hi, 2)),
            dma((1,)), dma((1,)), dma((max(1, n_hi - 1), max(1, (n_acq // 4 + n_acq // 8) * cap))), dma((n_hi,)),
        ],
        compiler_params=pltpu.CompilerParams(
            collective_id=0, has_side_effects=True, vmem_limit_bytes=VMEM_LIMIT * 2**20
        ),
    )(
        tile_slabs, dest_rank.reshape(1, subs), block_slot.reshape(1, subs),
        blend_weight.reshape(1, subs), shifts.T, parent_map.reshape(1, blocks),
    )
    return summed.reshape(PAR_DEV, 8, HZ, LANES)


def solution(mesh):
    placed = (P(("acq", "grp"), None, None), P(), P(), P(), P(), P(("acq", "grp")))
    return jax.shard_map(
        body,
        mesh=mesh,
        in_specs=placed,
        out_specs=P(("acq", "grp"), None, None, None),
        check_vma=False,
    )
```

```python
import functools
import jax
import jax.numpy as jnp
from jax import lax
from jax.experimental import pallas as pl
from jax.experimental.pallas import tpu as pltpu
from jax.sharding import PartitionSpec as P

BZ = 16
BY = 32
BX = 128
PAR_DEV = 2
HZ, HY, HX = BZ // 2, BY // 2, BX // 2
PAIRS = HY // 2
LANES = HY * HX
PER_LOAD = 2
VMEM_LIMIT = 62
MESH = pl.DeviceIdType.MESH


def flip(index, mask):
    out, bit = index, 1
    while bit < 64:
        out = out + bit * ((mask // bit) % 2) * (1 - 2 * ((index // bit) % 2))
        bit *= 2
    return out


def orders(count):
    unit = count // 4
    if unit < 1:
        plain = list(range(1, count))
        return plain, [[0] + plain] * 4
    half = unit - unit // 2
    side, near, far, farther = [list(range(q * unit, (q + 1) * unit)) for q in range(4)]
    side = side[1:]
    sends = side + near + far + farther
    arrivals = [
        [0] + side + far[:half] + near + far[half:] + farther,
        [0] + side + near[:half] + far[:half] + near[half:] + far[half:] + farther,
        [0] + far[:half] + side + far[half:] + near + farther,
        [0] + side + near[:half] + far[:half] + near[half:] + far[half:] + farther,
    ]
    return sends, arrivals


def layout(index, lo, count):
    sends, arrivals = orders(count)
    unit = max(1, count // 4)
    row = index // unit
    inner = (row + row // 2) % 2 if count >= 4 else 0

    def pick(*cases):
        if len(cases) == 2:
            return cases[0] + inner * (cases[1] - cases[0])
        below, above = pick(*cases[:2]), pick(*cases[2:])
        return below + lo * (above - below)

    def landing(d, within, low):
        if (d // unit) % 4 in (1, 2):
            within = 1 - within
        return arrivals[2 * low + within].index(d)

    targets = [
        (d, pick(*[landing(d, within, low) for low in range(2) for within in range(2)]))
        for d in sends
    ]
    return targets, [pick(*cases) for cases in zip(*arrivals)]


def halving_matrix():
    row = lax.broadcasted_iota(jnp.int32, (2 * BX, 2 * BX), 0)
    col = lax.broadcasted_iota(jnp.int32, (2 * BX, 2 * BX), 1)
    x, y = row % BX, row // BX
    cx, cy, part = col % HX, (col // HX) % 2, col // BX
    same = y == cy
    both = jnp.where(same & (x // 2 == cx), 1.0, 0.0)
    ahead = jnp.where(same & (x == jnp.minimum(2 * cx + 2, BX - 1)), 1.0, 0.0)
    here = jnp.where(same & (x == 2 * cx), 1.0, 0.0)
    return jnp.where(part == 0, both, ahead - here).astype(jnp.bfloat16)


def split(values):
    high = values.astype(jnp.bfloat16)
    return high, (values - high.astype(jnp.float32)).astype(jnp.bfloat16)


def kernel(
    n_acq, n_grp, cap, tile_hbm, dest_hbm, slot_hbm, weight_hbm, shift_hbm, parent_hbm, out,
    named_by, weight, shift, parent, named_rows, weight_row,
    tile, thin, high, low, half, factor, send, gath, named,
    meta_sem, load_sem, send_a, recv_a, send_x, recv_x, send_c, recv_c, send_p, recv_p, recv_r, recv_s, known,
):
    count = tile.shape[0]
    a, g = lax.axis_index("acq"), lax.axis_index("grp")
    hi, lo = g // 2, g % 2
    mate = hi * 2 + (1 - lo)
    n_hi = n_grp // 2
    rows = PAIRS * HZ

    barrier = pltpu.get_barrier_semaphore()
    unit = max(1, n_acq // 4)
    straight = list(range(1, unit)) + list(range(unit, n_acq, unit))
    for d in straight:
        pl.semaphore_signal(barrier, inc=1, device_id=(flip(a, d), g), device_id_type=MESH)
    for d in range(1, n_grp):
        pl.semaphore_signal(barrier, inc=1, device_id=(a, (g + d) % n_grp), device_id_type=MESH)
    lent = n_acq // 4 + n_acq // 8

    dest, slot = named_by.at[0], named_by.at[1]
    metas = [
        pltpu.make_async_copy(start, end, meta_sem.at[i])
        for start, end, i in (
            (dest_hbm, dest, 0), (slot_hbm, slot, 0), (weight_hbm, weight, 1),
            (shift_hbm, shift, 2), (parent_hbm, parent, 3),
            (dest_hbm, named_rows.at[0], 4), (slot_hbm, named_rows.at[1], 4),
            (weight_hbm, weight_row, 5),
        )
    ]
    for meta in metas:
        meta.start()

    def load(i):
        some = pl.ds(i * PER_LOAD, PER_LOAD)
        return pltpu.make_async_copy(tile_hbm.at[some], tile.at[some], load_sem.at[i])

    for i in range(count // PER_LOAD):
        load(i).start()

    matrix = halving_matrix()
    last = lax.broadcasted_iota(jnp.int32, (HZ, BX), 0) == HZ - 1
    for pair, i in ((named_by, 0), (named_rows, 4)):
        pltpu.make_async_copy(pair, pair, meta_sem.at[i]).wait()
    for i in (2, 3, 4, 7):
        metas[i].wait()

    blocks = parent.shape[1]
    base = (a * n_grp + g) * count
    target = [dest[0, base + s] for s in range(count)]
    key = [target[s] * blocks + slot[0, base + s] for s in range(count)]
    subs = lax.broadcasted_iota(jnp.int32, weight_row.shape, 1)
    keys = jnp.where(
        (subs // count) % n_grp == g, named_rows[0] * blocks + named_rows[1], -1
    )
    for s in range(count):
        denom = jnp.sum(jnp.where(keys == key[s], weight_row[...], 0.0), axis=1, keepdims=True)
        factor[s] = jnp.broadcast_to(
            (0.125 * weight[0, base + s]) / jnp.maximum(denom, 1.0), (HZ, BX)
        )
    factor[count] = jnp.zeros((HZ, BX), jnp.float32)
    spot = []
    for s in range(count):
        at = target[s] * cap
        for before in range(s):
            at = at + jnp.where(target[before] == target[s], 1, 0)
        spot.append(at)

    chosen = []
    for place in range(n_acq * cap):
        s = count
        for i in range(count):
            s = jnp.where(spot[i] == place, i, s)
        chosen.append(s)

    def soften(s):
        fz, fy = shift[0, base + s], shift[1, base + s]

        def row(y):
            return tile[s, :, pl.ds(y * BX, BX)]

        here = row(0)
        for j in range(HY):
            odd = row(2 * j + 1)
            ahead = row(2 * j + 2) if j < HY - 1 else odd
            thin[s, j] = here + odd + fy * (ahead - here)
            here = ahead
        for j in range(HY):
            even = thin[s, j, pl.ds(0, HZ, stride=2), :]
            odd = thin[s, j, pl.ds(1, HZ, stride=2), :]
            ahead = jnp.where(last, odd, pltpu.roll(even, HZ - 1, 0))
            top, rest = split(even + odd + fz * (ahead - even))
            place = (pl.ds((j // 2) * HZ, HZ), pl.ds((j % 2) * BX, BX))
            high[s, place[0], place[1]] = top.astype(jnp.float32)
            low[s, place[0], place[1]] = rest.astype(jnp.float32)

    def halve(s):
        half[s] = jnp.dot(
            high[s].astype(jnp.bfloat16), matrix, preferred_element_type=jnp.float32
        ) + jnp.dot(low[s].astype(jnp.bfloat16), matrix, preferred_element_type=jnp.float32)

    def loaded(i, carry):
        load(i).wait()
        for s in range(PER_LOAD):
            soften(i * PER_LOAD + s)
        return carry

    lax.fori_loop(0, count // PER_LOAD, loaded, 0)
    for s in range(count):
        halve(s)

    half[count] = jnp.zeros((rows, 2 * BX), jnp.float32)

    for place in range(n_acq * cap):
        s = chosen[place]
        fx = shift[2, base + jnp.minimum(s, count - 1)]
        value = half[s, :, pl.ds(0, BX)] + fx * half[s, :, pl.ds(BX, BX)]
        scale = factor[s]
        for p in range(PAIRS):
            send[place, :, pl.ds(p * BX, BX)] = scale * value[p * HZ : (p + 1) * HZ]

    pl.semaphore_wait(barrier, len(straight) + n_grp - 1)
    for d in range(1, unit):
        pl.semaphore_signal(known.at[0], inc=1, device_id=(flip(a, d), g), device_id_type=MESH)

    targets, order = layout(a, lo, n_acq)
    total = n_acq * cap
    middle = total // 2
    shared = total - lent * cap
    received = [(i, cap) for i in range(cap, middle, cap)] + [(i, 1) for i in range(middle, shared)]
    groups, first = [(0, shared)], shared
    while first < total:
        size = max(1, total - cap - first)
        groups.append((first, size))
        first += size
    borrowed = list(range(shared, total))

    def landed(at, c):
        late = at // (n_acq // 2)
        return at + late * ((at - n_acq // 2) * (cap - 1) + c)

    def lent_at(i):
        return n_acq // 2 * (1 + cap) + i - shared

    def to_acq(d, at, c):
        sem, core = landed(at, c), g
        if d >= n_acq - lent:
            sem = lo * sem + (1 - lo) * lent_at(d * cap + c)
            core = g + 1 - lo
        peer = flip(a, d)
        return pltpu.make_async_remote_copy(
            src_ref=send.at[peer * cap + c], dst_ref=gath.at[g, at * cap + c],
            send_sem=send_a.at[0], recv_sem=recv_a.at[sem],
            device_id=(peer, core), device_id_type=MESH,
        )

    def from_acq(owner, i, size, sem):
        piece = gath.at[owner, pl.ds(i, size)]
        return pltpu.make_async_remote_copy(
            src_ref=piece, dst_ref=piece, send_sem=send_a.at[0], recv_sem=recv_a.at[sem],
            device_id=(flip(a, 1), g), device_id_type=MESH,
        )

    def along(owner, first, size, peer, send_sem, recv_sem):
        piece = gath.at[owner, pl.ds(first, size)]
        return pltpu.make_async_remote_copy(
            src_ref=piece, dst_ref=piece, send_sem=send_sem, recv_sem=recv_sem,
            device_id=(a, peer), device_id_type=MESH,
        )

    others = [((hi + d) % n_hi) * 2 + lo for d in range(1, n_hi)]
    origins = [((hi + n_hi - d) % n_hi) * 2 + lo for d in range(1, n_hi)]
    mates = [((hi + n_hi - d) % n_hi) * 2 + 1 - lo for d in range(1, n_hi)]

    def over_x(owner, first, size, peer, d):
        k = max(k for k, (start, _) in enumerate(groups) if start <= first)
        return along(owner, first, size, peer, send_x.at[d - 1], recv_x.at[d - 1, k])

    def to_mate(owner, first, size, d):
        return along(owner, first, size, mate, send_c.at[d], recv_c.at[d, first // middle])

    def take(i, size):
        from_acq(g, i, size, landed(i // cap, i % cap)).wait_recv()
        for d, peer in enumerate(others, 1):
            over_x(g, i, size, peer, d).start()
        to_mate(g, i, size, 0).start()

    def lent_x(owner, i, peer, d):
        return along(owner, i, 1, peer, send_x.at[d - 1], recv_r.at[d - 1, i - shared])

    def lent_back(owner, first, size, d):
        return along(owner, first, size, mate, send_c.at[d], recv_s.at[d])

    def lent_past(owner, peer, d):
        return along(owner, total - 1, 1, peer, send_x.at[d - 1], recv_s.at[d])

    def take_lent(i):
        from_acq(mate, i, 1, lent_at(i)).wait_recv()
        for d, peer in enumerate(others, 1):
            if i == total - 1:
                lent_past(mate, peer - 1, d).start()
            lent_x(mate, i, peer, d).start()
        lent_back(mate, i, 1, 0).start()

    def relay(first, size):
        for d, owner in enumerate(origins, 1):
            over_x(owner, first, size, mate, d).wait_recv()
            cut = min(max(middle - first, 0), size)
            for at, length in ((first, cut), (first + cut, size - cut)):
                if length:
                    to_mate(owner, at, length, d).start()

    def relay_lent(i):
        for d, owner in enumerate(mates, 1):
            lent_x(owner, i, mate, d).wait_recv()
            if i < total - 1:
                lent_back(owner, i, 1, d).start()

    def arrived(d, h):
        owner = [mate, *mates][d]
        if h == 0:
            to_mate(owner, 0, middle, d).wait_recv()
            return

        @pl.when(lo == 0)
        def _():
            to_mate(owner, middle, total - middle, d).wait_recv()

        @pl.when(lo == 1)
        def _():
            to_mate(owner, middle, shared - middle, d).wait_recv()

    for c in range(cap):
        gath[g, c] = send[a * cap + c]
    sooner = [(d, at) for d, at in targets if d in straight and d < n_acq - lent]
    later = [pair for pair in targets if pair not in sooner]
    for d, at in sooner:
        for c in range(cap):
            to_acq(d, at, c).start()
    for d, peer in enumerate(others, 1):
        over_x(g, 0, cap, peer, d).start()
    to_mate(g, 0, cap, 0).start()

    depth = n_acq * cap * HZ
    side = depth // 2
    tall = PAR_DEV * 8 * HZ
    lane = lax.broadcasted_iota(jnp.int32, (HZ, depth), 1)
    at_slot = (lane % side) // HZ

    found = [jnp.zeros((HZ, depth), jnp.int32)] * 2
    for p, d in enumerate(order):
        first = (flip(a, d) * n_grp + g) * count
        seen = 0
        slots = [0] * cap
        for s in range(count):
            hit = jnp.where(dest[0, first + s] == a, 1, 0)
            for c in range(cap):
                slots[c] = jnp.where(
                    (hit == 1) & (seen == c), slot[0, first + s], slots[c]
                )
            seen = seen + hit
        h = p // (n_acq // 2)
        for c in range(cap):
            at = p * cap + c - h * (side // HZ)
            found[h] = jnp.where(at_slot == at, parent[0, slots[c]], found[h])
    for h in range(2):
        named[0, h] = found[h]

    def telling(d, peer):
        return pltpu.make_async_remote_copy(
            src_ref=named.at[0], dst_ref=named.at[d],
            send_sem=send_p.at[0], recv_sem=recv_p.at[0],
            device_id=(a, peer), device_id_type=MESH,
        )

    for d in range(1, n_grp):
        telling(d, (g + d) % n_grp).start()

    if unit > 1:
        pl.semaphore_wait(known.at[0], unit - 1)

    @pl.when(lo == 1)
    def _():
        pl.semaphore_signal(known.at[1], inc=1, device_id=(a, mate), device_id_type=MESH)

    for d, at in later:
        if d == n_acq - lent:
            @pl.when(lo == 0)
            def _():
                pl.semaphore_wait(known.at[1], 1)
        for c in range(cap):
            to_acq(d, at, c).start()

    upright = lax.broadcasted_iota(jnp.int32, (tall, depth), 0) + g * tall
    across_lane = lax.broadcasted_iota(jnp.int32, (tall, depth), 1) % HZ

    def place_rows(owner, h):
        placing = jnp.where(
            named[(g + n_grp - owner) % n_grp, h, pl.ds(0, 1), :] * HZ + across_lane == upright, 1.0, 0.0
        ).astype(jnp.bfloat16)
        rows = gath[owner, pl.ds(h * (side // HZ), side // HZ)].reshape(side, LANES)
        return jnp.dot(
            placing, jnp.concatenate(split(rows), axis=0), preferred_element_type=jnp.float32
        )

    for i, size in received:
        take(i, size)

    @pl.when(lo == 1)
    def _():
        for i in range(shared, total - cap):
            take(i, 1)
        last = total - cap
        for i in range(shared, last - cap // 2):
            take_lent(i)
        for i in range(last, total):
            take(i, 1)
            for j in range(i - cap // 2, i - cap // 2 + 1):
                if j < last:
                    take_lent(j)
        for j in range(last, total):
            take_lent(j)

    relay(*groups[0])

    @pl.when(lo == 1)
    def _():
        relay(*groups[1])
        relay_lent(borrowed[0])

    others_named = named.at[pl.ds(1, n_grp - 1)]
    naming = pltpu.make_async_remote_copy(
        src_ref=others_named, dst_ref=others_named,
        send_sem=send_p.at[0], recv_sem=recv_p.at[0],
        device_id=(a, mate), device_id_type=MESH,
    )
    naming.wait_recv()
    out[...] = place_rows(g, 0)
    for owner in origins:
        out[...] += place_rows(owner, 0)
    arrived(0, 0)
    out[...] += place_rows(mate, 0)

    @pl.when(lo == 0)
    def _():
        lent_back(g, shared, total - shared, 0).wait_recv()

    out[...] += place_rows(g, 1)
    arrived(0, 1)
    out[...] += place_rows(mate, 1)
    for d, owner in enumerate(mates, 1):
        arrived(d, 0)
        out[...] += place_rows(owner, 0)

    @pl.when(lo == 1)
    def _():
        rest = borrowed[1:]
        for group in groups[2:]:
            relay(*group)
            if rest:
                relay_lent(rest.pop(0))
        for i in rest:
            relay_lent(i)

    for d, owner in enumerate(mates, 1):
        arrived(d, 1)
        out[...] += place_rows(owner, 1)

    @pl.when(lo == 0)
    def _():
        for d, owner in enumerate(origins, 1):
            lent_back(owner, shared, total - shared, d).wait_recv()

    for owner in origins:
        out[...] += place_rows(owner, 1)

    naming.wait_send()
    left = send.at[pl.ds(cap, total - cap)]
    pltpu.make_async_remote_copy(
        src_ref=left, dst_ref=left, send_sem=send_a.at[0], recv_sem=recv_a.at[0],
        device_id=(flip(a, 1), g), device_id_type=MESH,
    ).wait_send()
    sent = [send_x.at[d - 1] for d in range(1, n_hi)] + [send_c.at[d] for d in range(n_hi)]
    for sem in sent:
        along(g, 0, shared, mate, sem, recv_s.at[0]).wait_send()

    @pl.when(lo == 1)
    def _():
        for sem in sent:
            along(g, shared, total - shared, mate, sem, recv_s.at[0]).wait_send()
        lent_back(g, shared, total - shared, 0).wait_send()
        for d in range(1, n_hi):
            along(g, shared, total - shared, mate, send_x.at[d - 1], recv_s.at[d]).wait_send()
            lent_past(g, mate, d).wait_send()
            lent_back(g, shared, total - 1 - shared, d).wait_send()


def body(tile_slabs, dest_rank, block_slot, shifts, blend_weight, parent_map):
    n_acq, n_grp = lax.axis_size("acq"), lax.axis_size("grp")
    count = tile_slabs.shape[0]
    subs = dest_rank.shape[0]
    blocks = parent_map.shape[0]
    cap = max(2, 2 * count // n_acq)
    depth = n_acq * cap * HZ
    hbm = pl.BlockSpec(memory_space=pltpu.HBM)
    rows = PAIRS * HZ
    dma = pltpu.SemaphoreType.DMA
    n_hi = n_grp // 2
    pieces = n_acq * cap
    summed = pl.pallas_call(
        functools.partial(kernel, n_acq, n_grp, cap),
        out_shape=pltpu.VMEM((PAR_DEV * 8 * HZ, LANES), jnp.float32),
        in_specs=[hbm] * 6,
        out_specs=pl.BlockSpec(memory_space=pltpu.VMEM),
        scratch_shapes=[
            pltpu.SMEM((2, 1, subs), jnp.int32),
            pltpu.SMEM((1, subs), jnp.float32),
            pltpu.SMEM((3, subs), jnp.float32),
            pltpu.SMEM((1, blocks), jnp.int32),
            pltpu.VMEM((2, 1, subs), jnp.int32),
            pltpu.VMEM((1, subs), jnp.float32),
            pltpu.VMEM((count, BZ, BY * BX), jnp.float32),
            pltpu.VMEM((count, HY, BZ, BX), jnp.float32),
            pltpu.VMEM((count, rows, 2 * BX), jnp.float32),
            pltpu.VMEM((count, rows, 2 * BX), jnp.float32),
            pltpu.VMEM((count + 1, rows, 2 * BX), jnp.float32),
            pltpu.VMEM((count + 1, HZ, BX), jnp.float32),
            pltpu.VMEM((n_acq * cap, HZ, LANES), jnp.float32),
            pltpu.VMEM((n_grp, n_acq * cap, HZ, LANES), jnp.float32),
            pltpu.VMEM((n_grp, 2, HZ, depth), jnp.int32),
            dma((6,)), dma((count // PER_LOAD,)),
            dma((1,)), dma((n_acq // 2 * (1 + cap) + (n_acq // 4 + n_acq // 8) * cap,)),
            dma((max(1, n_hi - 1),)), dma((max(1, n_hi - 1), pieces.bit_length())),
            dma((n_hi,)), dma((n_hi, 2)),
            dma((1,)), dma((1,)), dma((max(1, n_hi - 1), max(1, (n_acq // 4 + n_acq // 8) * cap))), dma((n_hi,)),
            pltpu.SemaphoreType.REGULAR((2,)),
        ],
        compiler_params=pltpu.CompilerParams(
            collective_id=0, has_side_effects=True, vmem_limit_bytes=VMEM_LIMIT * 2**20
        ),
    )(
        tile_slabs, dest_rank.reshape(1, subs), block_slot.reshape(1, subs),
        blend_weight.reshape(1, subs), shifts.T, parent_map.reshape(1, blocks),
    )
    return summed.reshape(PAR_DEV, 8, HZ, LANES)


def solution(mesh):
    placed = (P(("acq", "grp"), None, None), P(), P(), P(), P(), P(("acq", "grp")))
    return jax.shard_map(
        body,
        mesh=mesh,
        in_specs=placed,
        out_specs=P(("acq", "grp"), None, None, None),
        check_vma=False,
    )
```

```python
import functools
import jax
import jax.numpy as jnp
from jax import lax
from jax.experimental import pallas as pl
from jax.experimental.pallas import tpu as pltpu
from jax.sharding import PartitionSpec as P

BZ = 16
BY = 32
BX = 128
PAR_DEV = 2
HZ, HY, HX = BZ // 2, BY // 2, BX // 2
PAIRS = HY // 2
LANES = HY * HX
PER_LOAD = 2
VMEM_LIMIT = 62
MESH = pl.DeviceIdType.MESH


def flip(index, mask):
    out, bit = index, 1
    while bit < 64:
        out = out + bit * ((mask // bit) % 2) * (1 - 2 * ((index // bit) % 2))
        bit *= 2
    return out


def orders(count):
    unit = count // 4
    if unit < 1:
        plain = list(range(1, count))
        return plain, [[0] + plain] * 4
    half = unit - unit // 2
    side, near, far, farther = [list(range(q * unit, (q + 1) * unit)) for q in range(4)]
    side = side[1:]
    sends = side + near + far + farther
    arrivals = [
        [0] + side + far[:half] + near + far[half:] + farther,
        [0] + side + near[:half] + far[:half] + near[half:] + far[half:] + farther,
        [0] + far[:half] + side + near[:half] + far[half:] + near[half:] + farther,
        [0] + side + near[:half] + far[:half] + near[half:] + far[half:] + farther,
    ]
    return sends, arrivals


def layout(index, lo, count):
    sends, arrivals = orders(count)
    unit = max(1, count // 4)
    row = index // unit
    inner = (row + row // 2) % 2 if count >= 4 else 0

    def pick(*cases):
        if len(cases) == 2:
            return cases[0] + inner * (cases[1] - cases[0])
        below, above = pick(*cases[:2]), pick(*cases[2:])
        return below + lo * (above - below)

    def landing(d, within, low):
        if (d // unit) % 4 in (1, 2):
            within = 1 - within
        return arrivals[2 * low + within].index(d)

    targets = [
        (d, pick(*[landing(d, within, low) for low in range(2) for within in range(2)]))
        for d in sends
    ]
    return targets, [pick(*cases) for cases in zip(*arrivals)]


def halving_matrix():
    row = lax.broadcasted_iota(jnp.int32, (2 * BX, 2 * BX), 0)
    col = lax.broadcasted_iota(jnp.int32, (2 * BX, 2 * BX), 1)
    x, y = row % BX, row // BX
    cx, cy, part = col % HX, (col // HX) % 2, col // BX
    same = y == cy
    both = jnp.where(same & (x // 2 == cx), 1.0, 0.0)
    ahead = jnp.where(same & (x == jnp.minimum(2 * cx + 2, BX - 1)), 1.0, 0.0)
    here = jnp.where(same & (x == 2 * cx), 1.0, 0.0)
    return jnp.where(part == 0, both, ahead - here).astype(jnp.bfloat16)


def split(values):
    high = values.astype(jnp.bfloat16)
    return high, (values - high.astype(jnp.float32)).astype(jnp.bfloat16)


def kernel(
    n_acq, n_grp, cap, tile_hbm, dest_hbm, slot_hbm, weight_hbm, shift_hbm, parent_hbm, out,
    named_by, weight, shift, parent, named_rows, weight_row,
    tile, thin, high, low, half, factor, send, gath, named,
    meta_sem, load_sem, send_a, recv_a, send_x, recv_x, send_c, recv_c, send_p, recv_p, recv_r, recv_s, known,
):
    count = tile.shape[0]
    a, g = lax.axis_index("acq"), lax.axis_index("grp")
    hi, lo = g // 2, g % 2
    mate = hi * 2 + (1 - lo)
    n_hi = n_grp // 2
    rows = PAIRS * HZ

    barrier = pltpu.get_barrier_semaphore()
    unit = max(1, n_acq // 4)
    straight = list(range(1, unit)) + list(range(unit, n_acq, unit))
    for d in straight:
        pl.semaphore_signal(barrier, inc=1, device_id=(flip(a, d), g), device_id_type=MESH)
    for d in range(1, n_grp):
        pl.semaphore_signal(barrier, inc=1, device_id=(a, (g + d) % n_grp), device_id_type=MESH)
    lent = n_acq // 4 + n_acq // 8

    dest, slot = named_by.at[0], named_by.at[1]
    metas = [
        pltpu.make_async_copy(start, end, meta_sem.at[i])
        for start, end, i in (
            (dest_hbm, dest, 0), (slot_hbm, slot, 0), (weight_hbm, weight, 1),
            (shift_hbm, shift, 2), (parent_hbm, parent, 3),
            (dest_hbm, named_rows.at[0], 4), (slot_hbm, named_rows.at[1], 4),
            (weight_hbm, weight_row, 5),
        )
    ]
    for meta in metas:
        meta.start()

    def load(i):
        some = pl.ds(i * PER_LOAD, PER_LOAD)
        return pltpu.make_async_copy(tile_hbm.at[some], tile.at[some], load_sem.at[i])

    for i in range(count // PER_LOAD):
        load(i).start()

    matrix = halving_matrix()
    last = lax.broadcasted_iota(jnp.int32, (HZ, BX), 0) == HZ - 1
    for pair, i in ((named_by, 0), (named_rows, 4)):
        pltpu.make_async_copy(pair, pair, meta_sem.at[i]).wait()
    for i in (2, 3, 4, 7):
        metas[i].wait()

    blocks = parent.shape[1]
    base = (a * n_grp + g) * count
    target = [dest[0, base + s] for s in range(count)]
    key = [target[s] * blocks + slot[0, base + s] for s in range(count)]
    subs = lax.broadcasted_iota(jnp.int32, weight_row.shape, 1)
    keys = jnp.where(
        (subs // count) % n_grp == g, named_rows[0] * blocks + named_rows[1], -1
    )
    for s in range(count):
        denom = jnp.sum(jnp.where(keys == key[s], weight_row[...], 0.0), axis=1, keepdims=True)
        factor[s] = jnp.broadcast_to(
            (0.125 * weight[0, base + s]) / jnp.maximum(denom, 1.0), (HZ, BX)
        )
    factor[count] = jnp.zeros((HZ, BX), jnp.float32)
    spot = []
    for s in range(count):
        at = target[s] * cap
        for before in range(s):
            at = at + jnp.where(target[before] == target[s], 1, 0)
        spot.append(at)

    chosen = []
    for place in range(n_acq * cap):
        s = count
        for i in range(count):
            s = jnp.where(spot[i] == place, i, s)
        chosen.append(s)

    def soften(s):
        fz, fy = shift[0, base + s], shift[1, base + s]

        def row(y):
            return tile[s, :, pl.ds(y * BX, BX)]

        here = row(0)
        for j in range(HY):
            odd = row(2 * j + 1)
            ahead = row(2 * j + 2) if j < HY - 1 else odd
            thin[s, j] = here + odd + fy * (ahead - here)
            here = ahead
        for j in range(HY):
            even = thin[s, j, pl.ds(0, HZ, stride=2), :]
            odd = thin[s, j, pl.ds(1, HZ, stride=2), :]
            ahead = jnp.where(last, odd, pltpu.roll(even, HZ - 1, 0))
            top, rest = split(even + odd + fz * (ahead - even))
            place = (pl.ds((j // 2) * HZ, HZ), pl.ds((j % 2) * BX, BX))
            high[s, place[0], place[1]] = top.astype(jnp.float32)
            low[s, place[0], place[1]] = rest.astype(jnp.float32)

    def halve(s):
        half[s] = jnp.dot(
            high[s].astype(jnp.bfloat16), matrix, preferred_element_type=jnp.float32
        ) + jnp.dot(low[s].astype(jnp.bfloat16), matrix, preferred_element_type=jnp.float32)

    def loaded(i, carry):
        load(i).wait()
        for s in range(PER_LOAD):
            soften(i * PER_LOAD + s)
        return carry

    lax.fori_loop(0, count // PER_LOAD, loaded, 0)
    for s in range(count):
        halve(s)

    half[count] = jnp.zeros((rows, 2 * BX), jnp.float32)

    for place in range(n_acq * cap):
        s = chosen[place]
        fx = shift[2, base + jnp.minimum(s, count - 1)]
        value = half[s, :, pl.ds(0, BX)] + fx * half[s, :, pl.ds(BX, BX)]
        scale = factor[s]
        for p in range(PAIRS):
            send[place, :, pl.ds(p * BX, BX)] = scale * value[p * HZ : (p + 1) * HZ]

    pl.semaphore_wait(barrier, len(straight) + n_grp - 1)
    for d in range(1, unit):
        pl.semaphore_signal(known.at[0], inc=1, device_id=(flip(a, d), g), device_id_type=MESH)

    targets, order = layout(a, lo, n_acq)
    total = n_acq * cap
    middle = total // 2
    shared = total - lent * cap
    received = [(i, cap) for i in range(cap, middle, cap)] + [(i, 1) for i in range(middle, shared)]
    groups, first = [(0, shared)], shared
    while first < total:
        size = max(1, total - cap - first)
        groups.append((first, size))
        first += size
    borrowed = list(range(shared, total))

    def landed(at, c):
        late = at // (n_acq // 2)
        return at + late * ((at - n_acq // 2) * (cap - 1) + c)

    def lent_at(i):
        return n_acq // 2 * (1 + cap) + i - shared

    def to_acq(d, at, c):
        sem, core = landed(at, c), g
        if d >= n_acq - lent:
            sem = lo * sem + (1 - lo) * lent_at(d * cap + c)
            core = g + 1 - lo
        peer = flip(a, d)
        return pltpu.make_async_remote_copy(
            src_ref=send.at[peer * cap + c], dst_ref=gath.at[g, at * cap + c],
            send_sem=send_a.at[0], recv_sem=recv_a.at[sem],
            device_id=(peer, core), device_id_type=MESH,
        )

    def from_acq(owner, i, size, sem):
        piece = gath.at[owner, pl.ds(i, size)]
        return pltpu.make_async_remote_copy(
            src_ref=piece, dst_ref=piece, send_sem=send_a.at[0], recv_sem=recv_a.at[sem],
            device_id=(flip(a, 1), g), device_id_type=MESH,
        )

    def along(owner, first, size, peer, send_sem, recv_sem):
        piece = gath.at[owner, pl.ds(first, size)]
        return pltpu.make_async_remote_copy(
            src_ref=piece, dst_ref=piece, send_sem=send_sem, recv_sem=recv_sem,
            device_id=(a, peer), device_id_type=MESH,
        )

    others = [((hi + d) % n_hi) * 2 + lo for d in range(1, n_hi)]
    origins = [((hi + n_hi - d) % n_hi) * 2 + lo for d in range(1, n_hi)]
    mates = [((hi + n_hi - d) % n_hi) * 2 + 1 - lo for d in range(1, n_hi)]

    def over_x(owner, first, size, peer, d):
        k = max(k for k, (start, _) in enumerate(groups) if start <= first)
        return along(owner, first, size, peer, send_x.at[d - 1], recv_x.at[d - 1, k])

    def to_mate(owner, first, size, d):
        return along(owner, first, size, mate, send_c.at[d], recv_c.at[d, first // middle])

    def take(i, size):
        from_acq(g, i, size, landed(i // cap, i % cap)).wait_recv()
        for d, peer in enumerate(others, 1):
            over_x(g, i, size, peer, d).start()
        to_mate(g, i, size, 0).start()

    def lent_x(owner, i, peer, d):
        return along(owner, i, 1, peer, send_x.at[d - 1], recv_r.at[d - 1, i - shared])

    def lent_back(owner, first, size, d):
        return along(owner, first, size, mate, send_c.at[d], recv_s.at[d])

    def lent_past(owner, peer, d):
        return along(owner, total - 1, 1, peer, send_x.at[d - 1], recv_s.at[d])

    def take_lent(i):
        from_acq(mate, i, 1, lent_at(i)).wait_recv()
        for d, peer in enumerate(others, 1):
            if i == total - 1:
                lent_past(mate, peer - 1, d).start()
            lent_x(mate, i, peer, d).start()
        lent_back(mate, i, 1, 0).start()

    def relay(first, size):
        for d, owner in enumerate(origins, 1):
            over_x(owner, first, size, mate, d).wait_recv()
            cut = min(max(middle - first, 0), size)
            for at, length in ((first, cut), (first + cut, size - cut)):
                if length:
                    to_mate(owner, at, length, d).start()

    def relay_lent(i):
        for d, owner in enumerate(mates, 1):
            lent_x(owner, i, mate, d).wait_recv()
            if i < total - 1:
                lent_back(owner, i, 1, d).start()

    def arrived(d, h):
        owner = [mate, *mates][d]
        if h == 0:
            to_mate(owner, 0, middle, d).wait_recv()
            return

        @pl.when(lo == 0)
        def _():
            to_mate(owner, middle, total - middle, d).wait_recv()

        @pl.when(lo == 1)
        def _():
            to_mate(owner, middle, shared - middle, d).wait_recv()

    for c in range(cap):
        gath[g, c] = send[a * cap + c]
    sooner = [(d, at) for d, at in targets if d in straight and d < n_acq - lent]
    later = [pair for pair in targets if pair not in sooner]
    for d, at in sooner:
        for c in range(cap):
            to_acq(d, at, c).start()
    for d, peer in enumerate(others, 1):
        over_x(g, 0, cap, peer, d).start()
    to_mate(g, 0, cap, 0).start()

    depth = n_acq * cap * HZ
    side = depth // 2
    tall = PAR_DEV * 8 * HZ
    lane = lax.broadcasted_iota(jnp.int32, (HZ, depth), 1)
    at_slot = (lane % side) // HZ

    found = [jnp.zeros((HZ, depth), jnp.int32)] * 2
    for p, d in enumerate(order):
        first = (flip(a, d) * n_grp + g) * count
        seen = 0
        slots = [0] * cap
        for s in range(count):
            hit = jnp.where(dest[0, first + s] == a, 1, 0)
            for c in range(cap):
                slots[c] = jnp.where(
                    (hit == 1) & (seen == c), slot[0, first + s], slots[c]
                )
            seen = seen + hit
        h = p // (n_acq // 2)
        for c in range(cap):
            at = p * cap + c - h * (side // HZ)
            found[h] = jnp.where(at_slot == at, parent[0, slots[c]], found[h])
    for h in range(2):
        named[0, h] = found[h]

    def telling(d, peer):
        return pltpu.make_async_remote_copy(
            src_ref=named.at[0], dst_ref=named.at[d],
            send_sem=send_p.at[0], recv_sem=recv_p.at[0],
            device_id=(a, peer), device_id_type=MESH,
        )

    for d in range(1, n_grp):
        telling(d, (g + d) % n_grp).start()

    if unit > 1:
        pl.semaphore_wait(known.at[0], unit - 1)

    @pl.when(lo == 1)
    def _():
        pl.semaphore_signal(known.at[1], inc=1, device_id=(a, mate), device_id_type=MESH)

    for d, at in later:
        if d == n_acq - lent:
            @pl.when(lo == 0)
            def _():
                pl.semaphore_wait(known.at[1], 1)
        for c in range(cap):
            to_acq(d, at, c).start()

    upright = lax.broadcasted_iota(jnp.int32, (tall, depth), 0) + g * tall
    across_lane = lax.broadcasted_iota(jnp.int32, (tall, depth), 1) % HZ

    def place_rows(owner, h):
        placing = jnp.where(
            named[(g + n_grp - owner) % n_grp, h, pl.ds(0, 1), :] * HZ + across_lane == upright, 1.0, 0.0
        ).astype(jnp.bfloat16)
        rows = gath[owner, pl.ds(h * (side // HZ), side // HZ)].reshape(side, LANES)
        return jnp.dot(
            placing, jnp.concatenate(split(rows), axis=0), preferred_element_type=jnp.float32
        )

    for i, size in received:
        take(i, size)

    @pl.when(lo == 1)
    def _():
        for i in range(shared, total - cap):
            take(i, 1)
        last = total - cap
        for i in range(shared, last - cap // 2):
            take_lent(i)
        for i in range(last, total):
            take(i, 1)
            for j in range(i - cap // 2, i - cap // 2 + 1):
                if j < last:
                    take_lent(j)
        for j in range(last, total):
            take_lent(j)

    relay(*groups[0])

    @pl.when(lo == 1)
    def _():
        relay(*groups[1])
        relay_lent(borrowed[0])

    others_named = named.at[pl.ds(1, n_grp - 1)]
    naming = pltpu.make_async_remote_copy(
        src_ref=others_named, dst_ref=others_named,
        send_sem=send_p.at[0], recv_sem=recv_p.at[0],
        device_id=(a, mate), device_id_type=MESH,
    )
    naming.wait_recv()
    out[...] = place_rows(g, 0)
    for owner in origins:
        out[...] += place_rows(owner, 0)
    arrived(0, 0)
    out[...] += place_rows(mate, 0)

    @pl.when(lo == 0)
    def _():
        lent_back(g, shared, total - shared, 0).wait_recv()

    out[...] += place_rows(g, 1)
    arrived(0, 1)
    out[...] += place_rows(mate, 1)
    for d, owner in enumerate(mates, 1):
        arrived(d, 0)
        out[...] += place_rows(owner, 0)

    @pl.when(lo == 1)
    def _():
        rest = borrowed[1:]
        for group in groups[2:]:
            relay(*group)
            if rest:
                relay_lent(rest.pop(0))
        for i in rest:
            relay_lent(i)

    for d, owner in enumerate(mates, 1):
        arrived(d, 1)
        out[...] += place_rows(owner, 1)

    @pl.when(lo == 0)
    def _():
        for d, owner in enumerate(origins, 1):
            lent_back(owner, shared, total - shared, d).wait_recv()

    for owner in origins:
        out[...] += place_rows(owner, 1)

    naming.wait_send()
    left = send.at[pl.ds(cap, total - cap)]
    pltpu.make_async_remote_copy(
        src_ref=left, dst_ref=left, send_sem=send_a.at[0], recv_sem=recv_a.at[0],
        device_id=(flip(a, 1), g), device_id_type=MESH,
    ).wait_send()
    sent = [send_x.at[d - 1] for d in range(1, n_hi)] + [send_c.at[d] for d in range(n_hi)]
    for sem in sent:
        along(g, 0, shared, mate, sem, recv_s.at[0]).wait_send()

    @pl.when(lo == 1)
    def _():
        for sem in sent:
            along(g, shared, total - shared, mate, sem, recv_s.at[0]).wait_send()
        lent_back(g, shared, total - shared, 0).wait_send()
        for d in range(1, n_hi):
            along(g, shared, total - shared, mate, send_x.at[d - 1], recv_s.at[d]).wait_send()
            lent_past(g, mate, d).wait_send()
            lent_back(g, shared, total - 1 - shared, d).wait_send()


def body(tile_slabs, dest_rank, block_slot, shifts, blend_weight, parent_map):
    n_acq, n_grp = lax.axis_size("acq"), lax.axis_size("grp")
    count = tile_slabs.shape[0]
    subs = dest_rank.shape[0]
    blocks = parent_map.shape[0]
    cap = max(2, 2 * count // n_acq)
    depth = n_acq * cap * HZ
    hbm = pl.BlockSpec(memory_space=pltpu.HBM)
    rows = PAIRS * HZ
    dma = pltpu.SemaphoreType.DMA
    n_hi = n_grp // 2
    pieces = n_acq * cap
    summed = pl.pallas_call(
        functools.partial(kernel, n_acq, n_grp, cap),
        out_shape=pltpu.VMEM((PAR_DEV * 8 * HZ, LANES), jnp.float32),
        in_specs=[hbm] * 6,
        out_specs=pl.BlockSpec(memory_space=pltpu.VMEM),
        scratch_shapes=[
            pltpu.SMEM((2, 1, subs), jnp.int32),
            pltpu.SMEM((1, subs), jnp.float32),
            pltpu.SMEM((3, subs), jnp.float32),
            pltpu.SMEM((1, blocks), jnp.int32),
            pltpu.VMEM((2, 1, subs), jnp.int32),
            pltpu.VMEM((1, subs), jnp.float32),
            pltpu.VMEM((count, BZ, BY * BX), jnp.float32),
            pltpu.VMEM((count, HY, BZ, BX), jnp.float32),
            pltpu.VMEM((count, rows, 2 * BX), jnp.float32),
            pltpu.VMEM((count, rows, 2 * BX), jnp.float32),
            pltpu.VMEM((count + 1, rows, 2 * BX), jnp.float32),
            pltpu.VMEM((count + 1, HZ, BX), jnp.float32),
            pltpu.VMEM((n_acq * cap, HZ, LANES), jnp.float32),
            pltpu.VMEM((n_grp, n_acq * cap, HZ, LANES), jnp.float32),
            pltpu.VMEM((n_grp, 2, HZ, depth), jnp.int32),
            dma((6,)), dma((count // PER_LOAD,)),
            dma((1,)), dma((n_acq // 2 * (1 + cap) + (n_acq // 4 + n_acq // 8) * cap,)),
            dma((max(1, n_hi - 1),)), dma((max(1, n_hi - 1), pieces.bit_length())),
            dma((n_hi,)), dma((n_hi, 2)),
            dma((1,)), dma((1,)), dma((max(1, n_hi - 1), max(1, (n_acq // 4 + n_acq // 8) * cap))), dma((n_hi,)),
            pltpu.SemaphoreType.REGULAR((2,)),
        ],
        compiler_params=pltpu.CompilerParams(
            collective_id=0, has_side_effects=True, vmem_limit_bytes=VMEM_LIMIT * 2**20
        ),
    )(
        tile_slabs, dest_rank.reshape(1, subs), block_slot.reshape(1, subs),
        blend_weight.reshape(1, subs), shifts.T, parent_map.reshape(1, blocks),
    )
    return summed.reshape(PAR_DEV, 8, HZ, LANES)


def solution(mesh):
    placed = (P(("acq", "grp"), None, None), P(), P(), P(), P(), P(("acq", "grp")))
    return jax.shard_map(
        body,
        mesh=mesh,
        in_specs=placed,
        out_specs=P(("acq", "grp"), None, None, None),
        check_vma=False,
    )
```
